256 devices in a mesh: sector: 16 (over z_lo, x, core), term: 16 (over z_hi, y).
Axes of the slice: x: 4, y: 4, z: 8 (z_hi: 4, z_lo: 2; z = z_hi * 2 + z_lo), core: 2. Of those that a mesh axis runs over, the one named last changes fastest.
Arguments:
- lanczos_vector: float32 [32, 512, 512], P('sector'), may hold values from -6 to 6
- left_block: bfloat16 [32, 64, 512, 512], P('sector', 'term'), may hold values from -0.375 to 0.375
- right_block: bfloat16 [32, 64, 512, 512], P('sector', 'term'), may hold values from -0.25 to 0.25
- left_energy: float32 [32, 512], P('sector'), may hold values from 0.5 to 4
- right_energy: float32 [32, 512], P('sector'), may hold values from 0.5 to 4
- sector_shifts: int32 [64], P('term'), may hold values from -1 to 1
- sector_sizes: int32 [32], P('sector'), may hold values from 128 to 512, as said below
Outputs:
- next_vector: float32 [32, 512, 512], P('sector', 'term')
- next_sigma: float32 [32, 512, 512], P('sector', 'term')
The draws below stay inside these ranges and needn't reach their ends.
Inputs may be any that keep to these rules, and one draw needn't show every extreme that they name: `sector_sizes`: each value is a multiple of 128; some sector has exactly 512.
All inputs are finite; a program needn't handle non-finite values.
Results may differ from the reference program's by a relative error of at most 0.0023.
Values may be sent and summed in bfloat16 or wider, within the bound.
A program may use at most 64 MiB of HBM per device.

```python
import math
import jax
import jax.numpy as jnp
from jax import lax

P_SIZE = 512
SECTORS = 32
TERMS = 64


def draw_sector_sizes(key, part):
    level_key = jax.random.fold_in(key, 11)
    full_key = jax.random.fold_in(key, 12)
    levels = jax.random.randint(level_key, (SECTORS,), 1, 5) * (P_SIZE // 4)
    full_sector = jax.random.randint(full_key, (), 0, SECTORS)
    return jnp.where(jnp.arange(SECTORS) == full_sector, P_SIZE, levels).astype(jnp.int32)


def set_ends(array, stream_key, smallest, top_value):
    longest = array.shape.index(max(array.shape))
    spots = []
    for shift in (0, 1):
        where = [jax.random.randint(jax.random.fold_in(stream_key, axis), (), 0, length) for axis, length in enumerate(array.shape)]
        where[longest] = (where[longest] + shift) % array.shape[longest]
        spots.append(tuple(where))
    return array.at[spots[0]].set(smallest).at[spots[1]].set(top_value)


def with_spikes(entries, rng, source, target, shards_of, factor):
    def block_of(position):
        return (jnp.arange(entries.shape[position]) // (entries.shape[position] // shards_of)).reshape((-1,) + (1,) * (entries.ndim - 1 - position))

    one_side = jax.random.permutation(rng, shards_of)[block_of(target)]
    far = (block_of(target) + shards_of // 2) % shards_of
    return jnp.where((block_of(source) == one_side) | (block_of(source) == far), factor * entries, entries)


def level_of(key, dims, shards, least, largest):
    loudness = 1.0
    for position, blocks in shards:
        steps = jax.random.uniform(jax.random.fold_in(jax.random.fold_in(key, 6), position), (blocks,), jnp.float32, least / len(shards), largest / len(shards))
        loudness = loudness * jnp.repeat(jnp.exp(steps), dims[position] // blocks).reshape((-1,) + (1,) * (len(dims) - 1 - position))
    return loudness


def scatter_about(own_key, shape, deviation, bound, pieces=(), held_as=jnp.bfloat16):
    entries = deviation * jax.random.normal(own_key, shape, jnp.float32)
    if pieces:
        entries = entries * level_of(own_key, shape, pieces, -0.22, 0.18)
    return jnp.clip(entries, -bound, bound).astype(held_as)


def bell_draw_with(key, shape, spread, limit, cuts, heavy, kind=jnp.bfloat16):
    entries = spread * jax.random.normal(key, shape, jnp.float32)
    if cuts:
        entries = entries * level_of(key, shape, cuts, -0.22, 0.18)
    return jnp.clip(with_spikes(entries, jax.random.fold_in(key, 3), *heavy), -limit, limit).astype(kind)


def setup_inputs(seed: int = 0) -> dict:
    seeds = jax.random.split(jax.random.key(seed), 8)
    lanczos_vector = scatter_about(seeds[0], (SECTORS, P_SIZE, P_SIZE), 1.0, 6.0, ((0, 16),), jnp.float32)
    left_block = bell_draw_with(seeds[1], (SECTORS, TERMS, P_SIZE, P_SIZE), P_SIZE ** -0.5, 0.375, ((0, 16), (1, 16)), (1, 2, 16, 2.0))
    right_block = scatter_about(seeds[2], (SECTORS, TERMS, P_SIZE, P_SIZE), P_SIZE ** -0.5, 0.25, ((0, 16), (1, 16)))
    left_energy = jnp.clip(jnp.exp(math.log(4.0) - 2.0794415 * jax.random.uniform(seeds[3], (SECTORS, P_SIZE), jnp.float32) ** level_of(seeds[3], (SECTORS, P_SIZE), ((0, 16),), -0.2, 0.2)), 0.5, 4.0)
    right_energy = jnp.clip(jnp.exp(math.log(4.0) - 2.0794415 * jax.random.uniform(seeds[4], (SECTORS, P_SIZE), jnp.float32) ** level_of(seeds[4], (SECTORS, P_SIZE), ((0, 16),), -0.2, 0.2)), 0.5, 4.0)
    sector_shifts = set_ends(jax.random.randint(seeds[5], (TERMS,), -1, 2), jax.random.fold_in(seeds[5], 1), -1, 1).astype(jnp.int32)
    sector_sizes = draw_sector_sizes(jax.random.fold_in(seeds[7], 71), 0)
    return dict(lanczos_vector=lanczos_vector, left_block=left_block, right_block=right_block, left_energy=left_energy, right_energy=right_energy, sector_shifts=sector_shifts, sector_sizes=sector_sizes)


def apply_hamiltonian(full_blocks, left_block, right_block, energies, live_mask, sector_shifts):
    rounded = full_blocks.astype(jnp.bfloat16)
    empty = jnp.zeros((1, P_SIZE, P_SIZE), jnp.bfloat16)
    padded = jnp.concatenate([empty, rounded, empty], axis=0)

    def one_sector(input_arrays):
        sector_id, left_operator_terms, right_operator_terms = input_arrays
        partner_ids = (sector_id + 1 + sector_shifts).astype(jnp.int32)
        paired_sectors = padded[partner_ids]
        left_blended = jnp.einsum('zxn,znq->zxq', left_operator_terms.astype(jnp.float32), paired_sectors.astype(jnp.float32)).astype(jnp.bfloat16)
        return jnp.einsum('njp,nwp->jw', left_blended.astype(jnp.float32), right_operator_terms.astype(jnp.float32))
    sector_labels = jnp.arange(SECTORS, dtype=jnp.int32)
    partials = lax.map(one_sector, (sector_labels, left_block, right_block))
    term_scale = float(TERMS) ** (-0.5)
    return live_mask * (energies * full_blocks + term_scale * partials)

def reference(lanczos_vector, left_block, right_block, left_energy, right_energy, sector_shifts, sector_sizes):
    sector_positions = jnp.arange(P_SIZE, dtype=jnp.int32)
    limits = sector_sizes[:, None, None]
    live_mask = ((sector_positions[None, :, None] < limits) & (sector_positions[None, None, :] < limits)).astype(jnp.float32)
    energies = left_energy[:, :, None] + right_energy[:, None, :]
    cell_count = float(SECTORS * P_SIZE * P_SIZE)
    start_vector = live_mask * lanczos_vector
    sigma = apply_hamiltonian(start_vector, left_block, right_block, energies, live_mask, sector_shifts)
    correlation = jnp.sum(start_vector * sigma) / cell_count
    norm_sq = jnp.sum(start_vector * start_vector) / cell_count
    ritz_value = correlation / (norm_sq + 1e-06)
    residual = sigma - ritz_value * start_vector
    next_vector = residual / jnp.sqrt(jnp.sum(residual * residual) / cell_count + 1e-06)
    next_sigma = apply_hamiltonian(next_vector, left_block, right_block, energies, live_mask, sector_shifts)
    return (next_vector, next_sigma)
```

```python
import functools

import jax
import jax.numpy as jnp
from jax import lax
from jax.experimental import pallas as pl
from jax.experimental.pallas import tpu as pltpu
from jax.sharding import Mesh
from jax.sharding import PartitionSpec as P

TERM = ("term_0", "term_1")
SECTOR = ("sector_0", "sector_1", "sector_2")
MESH = pl.DeviceIdType.MESH
F32, BF16 = jnp.float32, jnp.bfloat16
EPSILON = 1e-06
COPIES = 240


def fold(values):
    total = None
    for j in range(values.shape[0]):
        for r in range(0, values.shape[1], 8):
            for c in range(0, values.shape[2], 128):
                piece = values[j, r : r + 8, c : c + 128]
                total = piece if total is None else total + piece
    return total


def kernel(
    dims,
    shifts,
    sizes,
    left_energy,
    right_energy,
    v_hbm,
    left_hbm,
    right_hbm,
    next_out,
    sigma_out,
    v_full,
    v_rows,
    left,
    right,
    wide_v,
    wide_u,
    opp_tx,
    relay_rx,
    dir_tx,
    dir_rx,
    sum_tx,
    sum_rx,
    near,
    own,
    z_tx,
    z_rx,
    rows_f32,
    stat_tx,
    stat_rx,
    load_sem,
    send_sem,
    recv_sem,
):
    n_lo, n_x, n_core, n_z, n_y = dims
    terms = left.shape[1]
    span, width = v_rows.shape[1], v_rows.shape[2]
    n_sec = n_lo * n_x * n_core
    block = n_z * n_y * span
    scale = float(terms * n_z * n_y) ** (-0.5)
    cells = float(2 * n_sec * block * width)

    lo, x, core = [lax.axis_index(a) for a in SECTOR]
    z, y = [lax.axis_index(a) for a in TERM]
    sec = (lo * n_x + x) * n_core + core
    rank = z * n_y + y
    zs = [lax.rem(z + k, n_z) for k in range(n_z)]
    ys = [lax.rem(y + k, n_y) for k in range(n_y)]
    zp, zo, zm = zs[1], zs[2], zs[3]
    yp, yo, ym = ys[1], ys[2], ys[3]
    y_to = [{"term_1": yp}, {"term_1": ym}]
    z_to = [{"term_0": zp}, {"term_0": zm}]

    def sector_device(s):
        s = lax.rem(s, n_sec)
        return {
            "sector_0": s // (n_x * n_core),
            "sector_1": lax.rem(s // n_core, n_x),
            "sector_2": lax.rem(s, n_core),
        }

    below, above = sector_device(sec + n_sec - 1), sector_device(sec + 1)
    axes = [
        ("sector_2", n_core, core),
        ("sector_1", n_x, x),
        ("term_1", n_y, y),
        ("sector_0", n_lo, lo),
        ("term_0", n_z, z),
    ]

    loads = [pltpu.make_async_copy(v_hbm.at[:, rank], v_rows, load_sem.at[0])]
    for j in range(2):
        loads.append(pltpu.make_async_copy(v_hbm.at[j], v_full.at[j], load_sem.at[1 + j]))
    loads.append(pltpu.make_async_copy(left_hbm, left, load_sem.at[3]))
    loads.append(pltpu.make_async_copy(right_hbm, right, load_sem.at[4]))
    for load in loads:
        load.start()

    barrier = pltpu.get_barrier_semaphore()
    peers = [below, above]
    for name, size, me in axes:
        peers += [{name: lax.rem(me + k, size)} for k in range(1, size)]
    for peer in peers:
        pl.semaphore_signal(barrier, inc=1, device_id=peer, device_id_type=MESH)

    copies = {}

    def send(key, src, dst, to):
        index = len(copies)
        copies[key] = pltpu.make_async_remote_copy(
            src_ref=src,
            dst_ref=dst,
            send_sem=send_sem.at[index],
            recv_sem=recv_sem.at[index],
            device_id=to,
            device_id_type=MESH,
        )
        copies[key].start()

    def arrived(*keys):
        for key in keys:
            copies[key].wait_recv()

    def stat_send(run, stage):
        name, size, me = axes[stage]
        for k in range(1, size):
            send(
                ("stat", run, stage, k),
                stat_tx.at[run, stage],
                stat_rx.at[run, stage, k - 1],
                {name: lax.rem(me + k, size)},
            )

    def stat_sum(run, stage):
        size = axes[stage][1]
        total = stat_tx[run, stage]
        for k in range(1, size):
            arrived(("stat", run, stage, k))
            total = total + stat_rx[run, stage, k - 1]
        stat_tx[run, stage + 1] = total
        if stage + 1 < len(axes):
            stat_send(run, stage + 1)

    def total_of(run, which):
        return jnp.sum(stat_tx[run, len(axes), which], keepdims=True)

    row = lax.broadcasted_iota(jnp.int32, (span, width), 0) + rank * span
    col = lax.broadcasted_iota(jnp.int32, (span, width), 1)
    masks, energies = [], []
    for j in range(2):
        masks.append((row < sizes[j]) & (col < sizes[j]))
        le = jnp.where(row == col, left_energy[j : j + 1, :], 0.0)
        energies.append(jnp.sum(le, axis=1, keepdims=True) + right_energy[j : j + 1, :])

    zero = jnp.zeros((n_y, span, width), BF16)
    for k in range(n_z):
        wide_v[4, k] = zero
        wide_u[4, k] = zero
    pl.semaphore_wait(barrier, len(peers))
    for j in range(2):
        loads[1 + j].wait()
        for k in range(n_z * n_y):
            r = lax.broadcasted_iota(jnp.int32, (span, width), 0) + k * span
            keep = (r < sizes[j]) & (col < sizes[j])
            wide_v[1 + j, k // n_y, k % n_y] = jnp.where(keep, v_full[j, k], 0.0).astype(BF16)
        send(("halo", j), wide_v.at[1 + j], wide_v.at[3 if j == 0 else 0], below if j == 0 else above)

    loads[0].wait()
    squares, weighted = [], []
    for j in range(2):
        v = jnp.where(masks[j], v_rows[j], 0.0)
        v_rows[j] = v
        squares.append(v * v)
        weighted.append(v * v * energies[j])
    stat_tx[0, 0, 0] = fold(jnp.stack(squares))
    stat_tx[0, 0, 1] = fold(jnp.stack(weighted))
    stat_send(0, 0)

    slots = []
    for j in range(2):
        for t in range(terms):
            p = 1 + j + shifts[t]
            outside = ((sec == 0) & (p == 0)) | ((sec == n_sec - 1) & (p == 3))
            slots.append(jnp.where(outside, 4, p))

    def chunk(vector, j, yy):
        total = jnp.zeros((n_z * span, block), F32)
        for t in range(terms):
            rows = left[j, t, :, yy].reshape(n_z * span, block)
            paired = vector[slots[j * terms + t]].reshape(block, width)
            mixed = jnp.dot(rows, paired, preferred_element_type=F32).astype(BF16)
            total = total + lax.dot_general(
                mixed, right[j, t], (((1,), (1,)), ((), ())), preferred_element_type=F32
            )
        return total.reshape(n_z, span, block)

    def summed_terms(run, vector, between):
        order = [zo, zp, zm, z]
        for j in range(2):
            opp_tx[run, j] = chunk(vector, j, yo).astype(BF16)
        for k, zz in enumerate(order):
            for d in range(2):
                send(("relay", run, k, d), opp_tx.at[run, d, zz], relay_rx.at[run, d, zz], y_to[d])

        def direct(k):
            for d in range(2):
                send(("dir", run, k, d), dir_tx.at[run, d, order[k]], dir_rx.at[run, d, order[k]], y_to[d])

        between(0)
        dir_tx[run, 0] = chunk(vector, 1, yp).astype(BF16)
        dir_tx[run, 1] = chunk(vector, 0, ym).astype(BF16)
        direct(0)
        between(1)
        near[0] = chunk(vector, 0, yp)
        near[1] = chunk(vector, 1, ym)
        for k, zz in enumerate(order):
            if k:
                direct(k)
            for d in range(2):
                arrived(("relay", run, k, d))
                sum_tx[run, d, zz] = (near[d, zz] + relay_rx[run, d, zz].astype(F32)).astype(BF16)
                send(("sum", run, k, d), sum_tx.at[run, d, zz], sum_rx.at[run, d, zz], y_to[d])
        between(2)
        for j in range(2):
            own[j] = chunk(vector, j, y)
        between(3)

        def collect(k):
            zz = order[k]
            arrived(*[(kind, run, k, d) for kind in ("dir", "sum") for d in range(2)])
            first = own[0, zz] + sum_rx[run, 0, zz].astype(F32) + dir_rx[run, 1, zz].astype(F32)
            second = own[1, zz] + sum_rx[run, 1, zz].astype(F32) + dir_rx[run, 0, zz].astype(F32)
            return first, second

        def z_send(kind, d, value):
            z_tx[run, kind, d] = value.astype(BF16)
            send(("z", run, kind, d), z_tx.at[run, kind, d], z_rx.at[run, kind, d], z_to[d])

        first, second = collect(0)
        z_send(0, 0, first)
        z_send(0, 1, second)
        first, second = collect(1)
        z_send(1, 0, second)
        rows_f32[0] = first
        first, second = collect(2)
        z_send(1, 1, first)
        rows_f32[1] = second
        for d in range(2):
            arrived(("z", run, 0, d))
            z_send(2, d, rows_f32[d] + z_rx[run, 0, d].astype(F32))
        first, second = collect(3)
        arrived(*[("z", run, kind, d) for kind in (1, 2) for d in range(2)])
        first = first + z_rx[run, 2, 0].astype(F32) + z_rx[run, 1, 1].astype(F32)
        second = second + z_rx[run, 2, 1].astype(F32) + z_rx[run, 1, 0].astype(F32)
        return [first, second]

    loads[3].wait()
    loads[4].wait()
    arrived(("halo", 0), ("halo", 1))
    sums = summed_terms(0, wide_v, lambda step: stat_sum(0, step))
    stat_sum(0, 4)
    norm = total_of(0, 0) / cells
    shift = total_of(0, 1) / cells / (norm + EPSILON)

    crossed, squares = [], []
    for j in range(2):
        v = v_rows[j]
        sigma = jnp.where(masks[j], energies[j] * v + scale * sums[j], 0.0)
        u = sigma - shift * v
        wide_u[1 + j, z, y] = u.astype(BF16)
        sigma_out[j] = sigma
        next_out[j] = u
        crossed.append(u * v)
        squares.append(u * u)

    def rows_send(key, j, zz, yy, to):
        part = wide_u.at[1 + j, zz, yy]
        send(key, part, part, to)

    strips = [z, zm, zp, zo]
    across = [y, ym, yp, yo]

    def z_own():
        for first in (True, False):
            for d in range(2):
                j = d if first else 1 - d
                rows_send(("gz", d, j), j, z, y, z_to[d])

    def z_forward(d):
        arrived(("gz", d, d))
        rows_send(("gzf", d), d, zm if d == 0 else zp, y, z_to[d])

    def y_own(k):
        for first in (True, False):
            for d in range(2):
                j = d if first else 1 - d
                rows_send(("gy", k, d, j), j, strips[k], y, y_to[d])

    def y_forward(k):
        for d in range(2):
            arrived(("gy", k, d, d))
            rows_send(("gyf", k, d), d, strips[k], ym if d == 0 else yp, y_to[d])

    def y_rest(k):
        for d in range(2):
            arrived(("gy", k, d, 1 - d))

    def halo(k, m):
        for j in range(2):
            send(
                ("gh", k, m, j),
                wide_u.at[1 + j, strips[k], across[m]],
                wide_u.at[3 if j == 0 else 0, strips[k], across[m]],
                below if j == 0 else above,
            )

    z_own()
    y_own(0)
    halo(0, 0)
    stat_tx[1, 0, 0] = fold(jnp.stack(crossed))
    stat_tx[1, 0, 1] = fold(jnp.stack(squares))
    stat_send(1, 0)
    y_forward(0)
    y_rest(0)
    halo(0, 1)
    halo(0, 2)
    for d in range(2):
        z_forward(d)
    for d in range(2):
        arrived(("gz", d, 1 - d))
    y_own(1)
    y_own(2)
    halo(1, 0)
    halo(2, 0)
    for d in range(2):
        arrived(("gyf", 0, d))
    halo(0, 3)
    stat_sum(1, 0)
    for d in range(2):
        arrived(("gzf", d))
    y_own(3)
    halo(3, 0)
    for k in (1, 2):
        y_forward(k)
        y_rest(k)
        halo(k, 1)
        halo(k, 2)
    y_forward(3)
    y_rest(3)
    halo(3, 1)
    halo(3, 2)
    for k in (1, 2, 3):
        for d in range(2):
            arrived(("gyf", k, d))
        halo(k, 3)
    arrived(*[("gh", k, m, j) for k in range(4) for m in range(4) for j in range(2)])

    sums = summed_terms(1, wide_u, lambda step: stat_sum(1, step + 1))

    cross, square = total_of(1, 0) / cells, total_of(1, 1) / cells
    gap = (cross - shift * EPSILON) / (norm + EPSILON)
    residual_sq = square - 2.0 * gap * cross + gap * gap * norm
    inverse = 1.0 / jnp.sqrt(jnp.maximum(residual_sq, 0.0) + EPSILON)
    for j in range(2):
        u, sigma = next_out[j], sigma_out[j]
        next_out[j] = inverse * (u - gap * v_rows[j])
        applied = jnp.where(masks[j], energies[j] * u + scale * sums[j], 0.0)
        sigma_out[j] = inverse * (applied - gap * sigma)

    for copy in copies.values():
        copy.wait_send()


def on_device(
    dims, lanczos_vector, left_block, right_block, left_energy, right_energy, sector_shifts, sector_sizes
):
    n_z, n_y = dims[3:]
    sectors, block, width = lanczos_vector.shape
    terms = left_block.shape[1]
    span = block // (n_z * n_y)
    strips = (n_z, n_y, span)
    out = jax.ShapeDtypeStruct((sectors, span, width), F32)
    exchange = pltpu.VMEM((2, 2, n_z, span, width), BF16)
    vmem, smem = (pl.BlockSpec(memory_space=s) for s in (pltpu.VMEM, pltpu.SMEM))
    hbm = pl.BlockSpec(memory_space=pl.ANY)
    return pl.pallas_call(
        functools.partial(kernel, dims),
        out_shape=(out, out),
        in_specs=[smem, smem, vmem, vmem, hbm, hbm, hbm],
        out_specs=(vmem, vmem),
        scratch_shapes=[
            pltpu.VMEM((sectors, n_z * n_y, span, width), F32),
            pltpu.VMEM((sectors, span, width), F32),
            pltpu.VMEM((sectors, terms, *strips, width), BF16),
            pltpu.VMEM((sectors, terms, block, width), BF16),
            pltpu.VMEM((5, *strips, width), BF16),
            pltpu.VMEM((5, *strips, width), BF16),
            *[exchange] * 6,
            pltpu.VMEM((2, n_z, span, width), F32),
            pltpu.VMEM((2, n_z, span, width), F32),
            pltpu.VMEM((2, 3, 2, span, width), BF16),
            pltpu.VMEM((2, 3, 2, span, width), BF16),
            pltpu.VMEM((2, span, width), F32),
            pltpu.VMEM((2, 6, 2, 8, 128), F32),
            pltpu.VMEM((2, 5, 3, 2, 8, 128), F32),
            pltpu.SemaphoreType.DMA((5,)),
            pltpu.SemaphoreType.DMA((COPIES,)),
            pltpu.SemaphoreType.DMA((COPIES,)),
        ],
        compiler_params=pltpu.CompilerParams(collective_id=0, has_side_effects=True),
        name="davidson_step",
    )(
        sector_shifts,
        sector_sizes,
        left_energy,
        right_energy,
        lanczos_vector.reshape(sectors, n_z * n_y, span, width),
        left_block.reshape(sectors, terms, *strips, width),
        right_block,
    )


def solution(mesh):
    dims = (2, 4, 2, 4, 4)
    finer = Mesh(mesh.devices.reshape(*dims), (*SECTOR, *TERM))
    return jax.shard_map(
        functools.partial(on_device, dims),
        mesh=finer,
        in_specs=(
            P(SECTOR, None, None),
            P(SECTOR, TERM, None, None),
            P(SECTOR, TERM, None, None),
            P(SECTOR, None),
            P(SECTOR, None),
            P(TERM),
            P(SECTOR),
        ),
        out_specs=(P(SECTOR, TERM, None), P(SECTOR, TERM, None)),
        check_vma=False,
    )
```

```python
import functools

import jax
import jax.numpy as jnp
from jax import lax
from jax.experimental import pallas as pl
from jax.experimental.pallas import tpu as pltpu
from jax.sharding import Mesh
from jax.sharding import PartitionSpec as P

TERM = ("term_0", "term_1")
SECTOR = ("sector_0", "sector_1", "sector_2")
MESH = pl.DeviceIdType.MESH
F32, BF16 = jnp.float32, jnp.bfloat16
EPSILON = 1e-06
GROUPS, SOURCES = 66, 12


def fold(values):
    total = None
    for j in range(values.shape[0]):
        for r in range(0, values.shape[1], 8):
            for c in range(0, values.shape[2], 128):
                piece = values[j, r : r + 8, c : c + 128]
                total = piece if total is None else total + piece
    return total


def kernel(
    dims,
    shifts_hbm,
    sizes_hbm,
    left_energy_hbm,
    right_energy_hbm,
    v_hbm,
    left_hbm,
    right_hbm,
    next_out,
    sigma_out,
    shifts,
    sizes,
    left_energy,
    right_energy,
    v_full,
    v_rows,
    left,
    right,
    wide_v,
    wide_u,
    opp_tx,
    relay_rx,
    y_tx,
    y_rx,
    near,
    own,
    z_tx,
    z_rx,
    rows_f32,
    mixed,
    turned,
    stat_tx,
    stat_rx,
    load_sem,
    send_sem,
    recv_sem,
):
    n_lo, n_x, n_core, n_z, n_y = dims
    terms = left.shape[1]
    span, width = v_rows.shape[1], v_rows.shape[2]
    n_sec = n_lo * n_x * n_core
    block = n_z * n_y * span
    scale = float(terms * n_z * n_y) ** (-0.5)
    cells = float(2 * n_sec * block * width)

    lo, x, core = [lax.axis_index(a) for a in SECTOR]
    z, y = [lax.axis_index(a) for a in TERM]
    sec = (lo * n_x + x) * n_core + core
    rank = z * n_y + y
    zs = [lax.rem(z + k, n_z) for k in range(n_z)]
    ys = [lax.rem(y + k, n_y) for k in range(n_y)]
    zp, zo, zm = zs[1], zs[2], zs[3]
    yp, yo, ym = ys[1], ys[2], ys[3]
    y_next = [yp, ym]
    y_to = [{"term_1": yp}, {"term_1": ym}]
    z_to = [{"term_0": zp}, {"term_0": zm}]

    def sector_device(s):
        s = lax.rem(s, n_sec)
        return {
            "sector_0": s // (n_x * n_core),
            "sector_1": lax.rem(s // n_core, n_x),
            "sector_2": lax.rem(s, n_core),
        }

    beside = [sector_device(sec + n_sec - 1), sector_device(sec + 1)]


    def pair(i):
        return i + 1 - 2 * lax.rem(i, 2)

    stages = [
        {"sector_2": 1 - core},
        {"sector_1": pair(x)},
        {"sector_1": n_x - 1 - x},
        {"sector_0": 1 - lo},
        {"term_0": pair(z)},
        {"term_0": n_z - 1 - z},
        {"term_1": pair(y)},
        {"term_1": n_y - 1 - y},
    ]
    last_stage = [4, 8]

    barrier = pltpu.get_barrier_semaphore()
    peers = [*beside, *y_to, {"term_1": yo}, *z_to, *stages[1:4]]
    for peer in peers:
        pl.semaphore_signal(barrier, inc=1, device_id=peer, device_id_type=MESH)

    loads = [pltpu.make_async_copy(v_hbm.at[:, rank], v_rows, load_sem.at[0])]
    for j in range(2):
        loads.append(pltpu.make_async_copy(v_hbm.at[j], v_full.at[j], load_sem.at[1 + j]))
    small = [
        (sizes_hbm, sizes),
        (shifts_hbm, shifts),
        (left_energy_hbm, left_energy),
        (right_energy_hbm, right_energy),
    ]
    small = [pltpu.make_async_copy(a, b, load_sem.at[5 + i]) for i, (a, b) in enumerate(small)]
    for load in small:
        load.start()
    loads.append(pltpu.make_async_copy(left_hbm, left, load_sem.at[3]))
    loads.append(pltpu.make_async_copy(right_hbm, right, load_sem.at[4]))
    for load in loads:
        load.start()

    groups, sources = {}, {}

    def send(group, source, src, dst, to):
        pltpu.make_async_remote_copy(
            src_ref=src,
            dst_ref=dst,
            send_sem=send_sem.at[sources.setdefault(source, len(sources))],
            recv_sem=recv_sem.at[groups.setdefault(group, len(groups))],
            device_id=to,
            device_id_type=MESH,
        ).start()

    def arrived(group, like):
        pltpu.make_async_copy(like, like, recv_sem.at[groups[group]]).wait()

    def sent(source, like):
        pltpu.make_async_copy(like, like, send_sem.at[sources[source]]).wait()

    def stat_send(run, stage):
        send(
            ("stat", run, stage),
            ("stat", run),
            stat_tx.at[run, stage],
            stat_rx.at[run, stage],
            stages[stage],
        )

    def stat_sum(run, stage):
        arrived(("stat", run, stage), stat_rx.at[run, stage])
        stat_tx[run, stage + 1] = stat_tx[run, stage] + stat_rx[run, stage]
        if stage + 1 < last_stage[run]:
            stat_send(run, stage + 1)

    def total_of(run, which):
        return jnp.sum(stat_tx[run, last_stage[run], which], keepdims=True)

    for load in small:
        load.wait()
    row = lax.broadcasted_iota(jnp.int32, (span, width), 0) + rank * span
    col = lax.broadcasted_iota(jnp.int32, (span, width), 1)
    masks, energies = [], []
    for j in range(2):
        masks.append((row < sizes[j]) & (col < sizes[j]))
        le = jnp.where(row == col, left_energy[j : j + 1, :], 0.0)
        energies.append(jnp.sum(le, axis=1, keepdims=True) + right_energy[j : j + 1, :])

    zero = jnp.zeros((n_y, span, width), BF16)
    for k in range(n_z):
        wide_v[4, k] = zero
        wide_u[4, k] = zero
    pl.semaphore_wait(barrier, len(peers))
    for j in range(2):
        loads[1 + j].wait()
        for k in range(n_z * n_y):
            r = lax.broadcasted_iota(jnp.int32, (span, width), 0) + k * span
            keep = (r < sizes[j]) & (col < sizes[j])
            wide_v[2 + j, k // n_y, k % n_y] = jnp.where(keep, v_full[j, k], 0.0).astype(BF16)
        send("halo", "halo", wide_v.at[2 + j], wide_v.at[1 - j], beside[j])

    eye = (
        lax.broadcasted_iota(jnp.int32, (span, 128), 0)
        - lax.broadcasted_iota(jnp.int32, (span, 128), 1)
    )
    squares = jnp.zeros((8, 128), F32)
    weighted = jnp.zeros((8, 128), F32)
    for j in range(2):
        for k in range(n_z * n_y):
            at = k * span // 128 * 128
            le = jnp.where(eye == at - k * span, left_energy[j : j + 1, at : at + 128], 0.0)
            energy = jnp.sum(le, axis=1, keepdims=True) + right_energy[j : j + 1, :]
            r = lax.broadcasted_iota(jnp.int32, (span, width), 0) + k * span
            keep = (r < sizes[j]) & (col < sizes[j])
            v = jnp.where(keep, v_full[j, k], 0.0)
            squares = squares + fold((v * v)[None])
            weighted = weighted + fold((v * v * energy)[None])
    stat_tx[0, 0, 0] = squares
    stat_tx[0, 0, 1] = weighted
    stat_send(0, 0)
    loads[0].wait()
    for j in range(2):
        v_rows[j] = jnp.where(masks[j], v_rows[j], 0.0)

    loads[4].wait()
    half = 256
    ones = lax.broadcasted_iota(jnp.int32, (half, half), 0) == lax.broadcasted_iota(
        jnp.int32, (half, half), 1
    )
    ones = ones.astype(F32).astype(BF16)
    for j in range(2):
        for t in range(terms):
            for a in range(0, block, half):
                for b in range(0, width, half):
                    turned[j, t * width + b : t * width + b + half, a : a + half] = lax.dot_general(
                        ones,
                        right[j, t, a : a + half, b : b + half],
                        (((1,), (1,)), ((), ())),
                        preferred_element_type=F32,
                    ).astype(BF16)

    slots = []
    for j in range(2):
        for t in range(terms):
            p = 1 + j + shifts[t]
            outside = ((sec == 0) & (p == 0)) | ((sec == n_sec - 1) & (p == 3))
            slots.append(jnp.where(outside, 4, jnp.where(p == 0, 0, jnp.where(p == 3, 1, p + 1))))

    def chunk(vector, j, yy):
        for t in range(terms):
            rows = left[j, t, :, yy].reshape(n_z * span, block)
            paired = vector[slots[j * terms + t]].reshape(block, width)
            mixed[j, :, t * width : (t + 1) * width] = jnp.dot(
                rows, paired, preferred_element_type=F32
            ).astype(BF16)
        total = jnp.dot(mixed[j], turned[j], preferred_element_type=F32)
        return total.reshape(n_z, span, block)

    def summed_terms(run, vector, between):
        order = [zo, zp, zm, z]
        for d in range(2):
            opp_tx[run, d] = chunk(vector, d, yo).astype(BF16)
            for k, zz in enumerate(order):
                send(
                    ("relay", run, k),
                    ("relay", run),
                    opp_tx.at[run, d, zz],
                    relay_rx.at[run, d, zz],
                    y_to[d] if k else {"term_1": yo},
                )

        def y_send(k, kind, d):
            part = 2 * kind + d
            send(
                ("y", run, k),
                ("y", run),
                y_tx.at[run, part, order[k]],
                y_rx.at[run, part, order[k]],
                y_to[d],
            )

        def relay(k):
            zz = order[k]
            arrived(("relay", run, k), relay_rx.at[run, :, zz])
            for d in range(2):
                y_tx[run, 2 + d, zz] = (near[d, zz] + relay_rx[run, d, zz].astype(F32)).astype(BF16)
                y_send(k, 1, d)

        for d in range(2):
            y_tx[run, d] = chunk(vector, 1 - d, y_next[d]).astype(BF16)
            y_send(0, 0, d)
        for d in range(2):
            near[d] = chunk(vector, d, y_next[d])
            y_tx[run, 2 + d, zo] = near[d, zo].astype(BF16)
            y_send(0, 1, d)
        between(0)
        for k in range(1, n_z):
            for d in range(2):
                y_send(k, 0, d)
            if k < 3:
                own[k - 1] = chunk(vector, k - 1, y)
            relay(k)

        def collect(k):
            zz = order[k]
            arrived(("y", run, k), y_rx.at[run, :, zz])
            first = own[0, zz] + y_rx[run, 2, zz].astype(F32) + y_rx[run, 1, zz].astype(F32)
            second = own[1, zz] + y_rx[run, 3, zz].astype(F32) + y_rx[run, 0, zz].astype(F32)
            if k == 0:
                arrived(("relay", run, 0), relay_rx.at[run, :, zo])
                first = first + relay_rx[run, 0, zo].astype(F32)
                second = second + relay_rx[run, 1, zo].astype(F32)
            return first, second

        def z_send(kind, d, value):
            z_tx[run, kind, d] = value.astype(BF16)
            send(
                ("z", run, min(kind, 1), d if kind == 0 else 0),
                ("z", run),
                z_tx.at[run, kind, d],
                z_rx.at[run, kind, d],
                z_to[d],
            )

        first, second = collect(0)
        z_send(0, 0, first)
        z_send(0, 1, second)
        between(1)
        first, second = collect(1)
        z_send(1, 0, second)
        rows_f32[0] = first
        first, second = collect(2)
        z_send(1, 1, first)
        rows_f32[1] = second
        for d in range(2):
            arrived(("z", run, 0, d), z_rx.at[run, 0, d])
            z_send(2, d, rows_f32[d] + z_rx[run, 0, d].astype(F32))
        between(2)
        first, second = collect(3)
        arrived(("z", run, 1, 0), z_rx.at[run, 1:3])
        between(3)
        first = first + z_rx[run, 2, 0].astype(F32) + z_rx[run, 1, 1].astype(F32)
        second = second + z_rx[run, 2, 1].astype(F32) + z_rx[run, 1, 0].astype(F32)
        return [first, second]

    loads[3].wait()
    arrived("halo", wide_v.at[0:2])
    sums = summed_terms(0, wide_v, lambda step: stat_sum(0, step))
    norm = total_of(0, 0) / cells
    shift = total_of(0, 1) / cells / (norm + EPSILON)

    crossed, squares = [], []
    for j in range(2):
        v = v_rows[j]
        sigma = jnp.where(masks[j], energies[j] * v + scale * sums[j], 0.0)
        u = sigma - shift * v
        wide_u[2 + j, z, y] = u.astype(BF16)
        sigma_out[j] = sigma
        next_out[j] = u
        crossed.append(u * v)
        squares.append(u * u)

    def rows_send(group, source, j, zz, yy, to):
        part = wide_u.at[2 + j, zz, yy]
        send(group, source, part, part, to)

    strips = [z, zm, zp, zo]
    across = [y, ym, yp, yo]

    def rows_arrived(group, j, zz, yy):
        arrived(group, wide_u.at[2 + j, zz, yy])

    def z_forward(d):
        zz = (zm, zp)[d]
        rows_arrived(("gz", d, d), d, zz, y)
        rows_send(("gzf", d), "gz", d, zz, y, z_to[d])

    def y_own(k):
        for first in (True, False):
            for d in range(2):
                j = d if first else 1 - d
                rows_send(("gy", k, d, j), "gy", j, strips[k], y, y_to[d])

    def y_forward(k):
        for d in range(2):
            rows_arrived(("gy", k, d, d), d, strips[k], (ym, yp)[d])
            rows_send(("gyf", k, d), "gy", d, strips[k], (ym, yp)[d], y_to[d])

    def y_rest(k):
        for d in range(2):
            rows_arrived(("gy", k, d, 1 - d), 1 - d, strips[k], (ym, yp)[d])

    def y_last(k):
        for d in range(2):
            rows_arrived(("gyf", k, d), d, strips[k], yo)

    def halo(k, m):
        for j in range(2):
            part = (strips[k], across[m])
            send("gh", "gh", wide_u.at[2 + j, *part], wide_u.at[1 - j, *part], beside[j])

    for first in (True, False):
        for d in range(2):
            j = d if first else 1 - d
            rows_send(("gz", d, j), "gz", j, z, y, z_to[d])
    y_own(0)
    halo(0, 0)
    stat_tx[1, 0, 0] = fold(jnp.stack(crossed))
    stat_tx[1, 0, 1] = fold(jnp.stack(squares))
    stat_send(1, 0)
    y_forward(0)
    y_rest(0)
    halo(0, 1)
    halo(0, 2)
    for d in range(2):
        z_forward(d)
    for d in range(2):
        rows_arrived(("gz", d, 1 - d), 1 - d, (zm, zp)[d], y)
    y_own(1)
    y_own(2)
    halo(1, 0)
    halo(2, 0)
    stat_sum(1, 0)
    y_last(0)
    halo(0, 3)
    for d in range(2):
        rows_arrived(("gzf", d), d, zo, y)
    for j in range(2):
        rows_send(("gyf", 3, j), "gy", j, zo, y, {"term_1": yo})
    y_own(3)
    halo(3, 0)
    stat_sum(1, 1)
    for k in (1, 2):
        y_forward(k)
        y_rest(k)
        halo(k, 1)
        halo(k, 2)
    for d in range(2):
        rows_arrived(("gy", 3, d, d), d, zo, (ym, yp)[d])
    y_rest(3)
    halo(3, 1)
    halo(3, 2)
    stat_sum(1, 2)
    for k in (1, 2, 3):
        y_last(k)
        halo(k, 3)
    stat_sum(1, 3)
    arrived("gh", wide_u.at[0:2])

    sums = summed_terms(1, wide_u, lambda step: stat_sum(1, step + 4))

    cross, square = total_of(1, 0) / cells, total_of(1, 1) / cells
    gap = (cross - shift * EPSILON) / (norm + EPSILON)
    residual_sq = square - 2.0 * gap * cross + gap * gap * norm
    inverse = 1.0 / jnp.sqrt(jnp.maximum(residual_sq, 0.0) + EPSILON)
    for j in range(2):
        u, sigma = next_out[j], sigma_out[j]
        next_out[j] = inverse * (u - gap * v_rows[j])
        applied = jnp.where(masks[j], energies[j] * u + scale * sums[j], 0.0)
        sigma_out[j] = inverse * (applied - gap * sigma)

    sent("halo", wide_v.at[2:4])
    for run in range(2):
        sent(("relay", run), opp_tx.at[run])
        sent(("y", run), y_tx.at[run])
        sent(("z", run), z_tx.at[run])
        sent(("stat", run), stat_tx.at[run, 0 : last_stage[run]])
    sent("gz", z_tx.at[0])
    sent("gy", left.at[0, 0:2, 0:3])
    sent("gh", wide_u.at[2:4])


def on_device(
    dims, lanczos_vector, left_block, right_block, left_energy, right_energy, sector_shifts, sector_sizes
):
    n_z, n_y = dims[3:]
    sectors, block, width = lanczos_vector.shape
    terms = left_block.shape[1]
    span = block // (n_z * n_y)
    strips = (n_z, n_y, span)
    out = pltpu.VMEM((sectors, span, width), F32)
    exchange = [pltpu.VMEM((2, parts, n_z, span, width), BF16) for parts in (2, 2, 4, 4)]
    vmem = pl.BlockSpec(memory_space=pltpu.VMEM)
    hbm = pl.BlockSpec(memory_space=pl.ANY)
    return pl.pallas_call(
        functools.partial(kernel, dims),
        out_shape=(out, out),
        in_specs=[hbm] * 7,
        out_specs=(vmem, vmem),
        scratch_shapes=[
            pltpu.SMEM((terms,), jnp.int32),
            pltpu.SMEM((sectors,), jnp.int32),
            pltpu.VMEM((sectors, block), F32),
            pltpu.VMEM((sectors, width), F32),
            pltpu.VMEM((sectors, n_z * n_y, span, width), F32),
            pltpu.VMEM((sectors, span, width), F32),
            pltpu.VMEM((sectors, terms, *strips, width), BF16),
            pltpu.VMEM((sectors, terms, block, width), BF16),
            pltpu.VMEM((5, *strips, width), BF16),
            pltpu.VMEM((5, *strips, width), BF16),
            *exchange,
            pltpu.VMEM((2, n_z, span, width), F32),
            pltpu.VMEM((2, n_z, span, width), F32),
            pltpu.VMEM((2, 3, 2, span, width), BF16),
            pltpu.VMEM((2, 3, 2, span, width), BF16),
            pltpu.VMEM((2, span, width), F32),
            pltpu.VMEM((sectors, n_z * span, terms * width), BF16),
            pltpu.VMEM((sectors, terms * width, block), BF16),
            pltpu.VMEM((2, 9, 2, 8, 128), F32),
            pltpu.VMEM((2, 8, 2, 8, 128), F32),
            pltpu.SemaphoreType.DMA((9,)),
            pltpu.SemaphoreType.DMA((SOURCES,)),
            pltpu.SemaphoreType.DMA((GROUPS,)),
        ],
        compiler_params=pltpu.CompilerParams(collective_id=0, has_side_effects=True),
        name="davidson_step",
    )(
        sector_shifts,
        sector_sizes,
        left_energy,
        right_energy,
        lanczos_vector.reshape(sectors, n_z * n_y, span, width),
        left_block.reshape(sectors, terms, *strips, width),
        right_block,
    )


def solution(mesh):
    dims = (2, 4, 2, 4, 4)
    finer = Mesh(mesh.devices.reshape(*dims), (*SECTOR, *TERM))
    return jax.shard_map(
        functools.partial(on_device, dims),
        mesh=finer,
        in_specs=(
            P(SECTOR, None, None),
            P(SECTOR, TERM, None, None),
            P(SECTOR, TERM, None, None),
            P(SECTOR, None),
            P(SECTOR, None),
            P(TERM),
            P(SECTOR),
        ),
        out_specs=(P(SECTOR, TERM, None), P(SECTOR, TERM, None)),
        check_vma=False,
    )
```

```python
import functools

import jax
import jax.numpy as jnp
from jax import lax
from jax.experimental import pallas as pl
from jax.experimental.pallas import tpu as pltpu
from jax.sharding import Mesh
from jax.sharding import PartitionSpec as P

TERM = ("term_0", "term_1")
SECTOR = ("sector_0", "sector_1", "sector_2")
MESH = pl.DeviceIdType.MESH
F32, BF16 = jnp.float32, jnp.bfloat16
EPSILON = 1e-06
GROUPS, SOURCES = 66, 13


def fold(values):
    total = None
    for j in range(values.shape[0]):
        for r in range(0, values.shape[1], 8):
            for c in range(0, values.shape[2], 128):
                piece = values[j, r : r + 8, c : c + 128]
                total = piece if total is None else total + piece
    return total


def kernel(
    dims,
    shifts_hbm,
    sizes_hbm,
    left_energy_hbm,
    right_energy_hbm,
    v_hbm,
    left_hbm,
    right_hbm,
    next_out,
    sigma_out,
    shifts,
    sizes,
    left_energy,
    right_energy,
    v_full,
    v_rows,
    left,
    right,
    wide_v,
    wide_u,
    opp_tx,
    relay_rx,
    y_tx,
    y_rx,
    near,
    own,
    z_tx,
    z_rx,
    rows_f32,
    mixed,
    turned,
    stat_tx,
    stat_rx,
    load_sem,
    send_sem,
    recv_sem,
):
    n_lo, n_x, n_core, n_z, n_y = dims
    terms = left.shape[1]
    span, width = v_rows.shape[1], v_rows.shape[2]
    n_sec = n_lo * n_x * n_core
    block = n_z * n_y * span
    scale = float(terms * n_z * n_y) ** (-0.5)
    cells = float(2 * n_sec * block * width)

    lo, x, core = [lax.axis_index(a) for a in SECTOR]
    z, y = [lax.axis_index(a) for a in TERM]
    sec = (lo * n_x + x) * n_core + core
    rank = z * n_y + y
    zs = [lax.rem(z + k, n_z) for k in range(n_z)]
    ys = [lax.rem(y + k, n_y) for k in range(n_y)]
    zp, zo, zm = zs[1], zs[2], zs[3]
    yp, yo, ym = ys[1], ys[2], ys[3]
    y_next = [yp, ym]
    y_to = [{"term_1": yp}, {"term_1": ym}]
    z_to = [{"term_0": zp}, {"term_0": zm}]

    def sector_device(s):
        s = lax.rem(s, n_sec)
        return {
            "sector_0": s // (n_x * n_core),
            "sector_1": lax.rem(s // n_core, n_x),
            "sector_2": lax.rem(s, n_core),
        }

    beside = [sector_device(sec + n_sec - 1), sector_device(sec + 1)]
    outer = sector_device(sec + n_sec - 1 + 2 * core)
    outer = [{**outer, "term_1": yy} for yy in ys[1:]]


    def pair(i):
        return i + 1 - 2 * lax.rem(i, 2)

    stages = [
        {"sector_1": pair(x)},
        {"sector_1": n_x - 1 - x},
        {"sector_2": 1 - core},
        {"sector_0": 1 - lo},
        {"term_0": pair(z)},
        {"term_0": n_z - 1 - z},
        {"term_1": pair(y)},
        {"term_1": n_y - 1 - y},
    ]
    last_stage = [4, 8]

    barrier = pltpu.get_barrier_semaphore()
    peers = [*beside, *y_to, {"term_1": yo}, *z_to, *outer, *stages[:2], stages[3]]
    for peer in peers:
        pl.semaphore_signal(barrier, inc=1, device_id=peer, device_id_type=MESH)

    loads = [pltpu.make_async_copy(v_hbm.at[:, rank], v_rows, load_sem.at[0])]
    for j in range(2):
        loads.append(pltpu.make_async_copy(v_hbm.at[j], v_full.at[j], load_sem.at[1 + j]))
    small = [
        (sizes_hbm, sizes),
        (shifts_hbm, shifts),
        (left_energy_hbm, left_energy),
        (right_energy_hbm, right_energy),
    ]
    small = [pltpu.make_async_copy(a, b, load_sem.at[5 + i]) for i, (a, b) in enumerate(small)]
    for load in small:
        load.start()
    loads.append(pltpu.make_async_copy(left_hbm, left, load_sem.at[3]))
    loads.append(pltpu.make_async_copy(right_hbm, right, load_sem.at[4]))
    for load in loads:
        load.start()

    groups, sources = {}, {}

    def send(group, source, src, dst, to):
        pltpu.make_async_remote_copy(
            src_ref=src,
            dst_ref=dst,
            send_sem=send_sem.at[sources.setdefault(source, len(sources))],
            recv_sem=recv_sem.at[groups.setdefault(group, len(groups))],
            device_id=to,
            device_id_type=MESH,
        ).start()

    def arrived(group, like):
        pltpu.make_async_copy(like, like, recv_sem.at[groups[group]]).wait()

    def sent(source, like):
        pltpu.make_async_copy(like, like, send_sem.at[sources[source]]).wait()

    def stat_send(run, stage):
        send(
            ("stat", run, stage),
            ("stat", run),
            stat_tx.at[run, stage],
            stat_rx.at[run, stage],
            stages[stage],
        )

    def stat_sum(run, stage):
        arrived(("stat", run, stage), stat_rx.at[run, stage])
        stat_tx[run, stage + 1] = stat_tx[run, stage] + stat_rx[run, stage]
        if stage + 1 < last_stage[run]:
            stat_send(run, stage + 1)

    def total_of(run, which):
        return jnp.sum(stat_tx[run, last_stage[run], which], keepdims=True)

    for load in small:
        load.wait()
    row = lax.broadcasted_iota(jnp.int32, (span, width), 0) + rank * span
    col = lax.broadcasted_iota(jnp.int32, (span, width), 1)
    masks, energies = [], []
    for j in range(2):
        masks.append((row < sizes[j]) & (col < sizes[j]))
        le = jnp.where(row == col, left_energy[j : j + 1, :], 0.0)
        energies.append(jnp.sum(le, axis=1, keepdims=True) + right_energy[j : j + 1, :])

    zero = jnp.zeros((n_y, span, width), BF16)
    for k in range(n_z):
        wide_v[4, k] = zero
        wide_u[4, k] = zero
    pl.semaphore_wait(barrier, len(peers))
    for j in range(2):
        loads[1 + j].wait()
        for k in range(n_z * n_y):
            r = lax.broadcasted_iota(jnp.int32, (span, width), 0) + k * span
            keep = (r < sizes[j]) & (col < sizes[j])
            wide_v[2 + j, k // n_y, k % n_y] = jnp.where(keep, v_full[j, k], 0.0).astype(BF16)
        send("halo", "halo", wide_v.at[2 + j], wide_v.at[1 - j], beside[j])

    eye = (
        lax.broadcasted_iota(jnp.int32, (span, 128), 0)
        - lax.broadcasted_iota(jnp.int32, (span, 128), 1)
    )
    squares = jnp.zeros((8, 128), F32)
    weighted = jnp.zeros((8, 128), F32)
    for j in range(2):
        for k in range(n_z * n_y):
            at = k * span // 128 * 128
            le = jnp.where(eye == at - k * span, left_energy[j : j + 1, at : at + 128], 0.0)
            energy = jnp.sum(le, axis=1, keepdims=True) + right_energy[j : j + 1, :]
            r = lax.broadcasted_iota(jnp.int32, (span, width), 0) + k * span
            keep = (r < sizes[j]) & (col < sizes[j])
            v = jnp.where(keep, v_full[j, k], 0.0)
            squares = squares + fold((v * v)[None])
            weighted = weighted + fold((v * v * energy)[None])
    stat_tx[0, 0, 0] = squares
    stat_tx[0, 0, 1] = weighted
    stat_send(0, 0)
    loads[0].wait()
    for j in range(2):
        v_rows[j] = jnp.where(masks[j], v_rows[j], 0.0)

    loads[4].wait()
    half = 256
    ones = lax.broadcasted_iota(jnp.int32, (half, half), 0) == lax.broadcasted_iota(
        jnp.int32, (half, half), 1
    )
    ones = ones.astype(F32).astype(BF16)
    for j in range(2):
        for t in range(terms):
            for a in range(0, block, half):
                for b in range(0, width, half):
                    turned[j, t * width + b : t * width + b + half, a : a + half] = lax.dot_general(
                        ones,
                        right[j, t, a : a + half, b : b + half],
                        (((1,), (1,)), ((), ())),
                        preferred_element_type=F32,
                    ).astype(BF16)

    slots = []
    for j in range(2):
        for t in range(terms):
            p = 1 + j + shifts[t]
            outside = ((sec == 0) & (p == 0)) | ((sec == n_sec - 1) & (p == 3))
            slots.append(jnp.where(outside, 4, jnp.where(p == 0, 0, jnp.where(p == 3, 1, p + 1))))

    def chunk(vector, j, yy):
        for t in range(terms):
            rows = left[j, t, :, yy].reshape(n_z * span, block)
            paired = vector[slots[j * terms + t]].reshape(block, width)
            mixed[j, :, t * width : (t + 1) * width] = jnp.dot(
                rows, paired, preferred_element_type=F32
            ).astype(BF16)
        total = jnp.dot(mixed[j], turned[j], preferred_element_type=F32)
        return total.reshape(n_z, span, block)

    def summed_terms(run, vector, between):
        order = [zo, zp, zm, z]
        for d in range(2):
            opp_tx[run, d] = chunk(vector, d, yo).astype(BF16)
            for k, zz in enumerate(order):
                send(
                    ("relay", run, k),
                    ("relay", run),
                    opp_tx.at[run, d, zz],
                    relay_rx.at[run, d, zz],
                    y_to[d] if k else {"term_1": yo},
                )

        def y_send(k, kind, d):
            part = 2 * kind + d
            send(
                ("y", run, k),
                ("y", run),
                y_tx.at[run, part, order[k]],
                y_rx.at[run, part, order[k]],
                y_to[d],
            )

        def relay(k):
            zz = order[k]
            arrived(("relay", run, k), relay_rx.at[run, :, zz])
            for d in range(2):
                y_tx[run, 2 + d, zz] = (near[d, zz] + relay_rx[run, d, zz].astype(F32)).astype(BF16)
                y_send(k, 1, d)

        for d in range(2):
            y_tx[run, d] = chunk(vector, 1 - d, y_next[d]).astype(BF16)
            y_send(0, 0, d)
        for d in range(2):
            near[d] = chunk(vector, d, y_next[d])
            y_tx[run, 2 + d, zo] = near[d, zo].astype(BF16)
            y_send(0, 1, d)
        between(0)
        for k in range(1, n_z):
            for d in range(2):
                y_send(k, 0, d)
            if k < 3:
                own[k - 1] = chunk(vector, k - 1, y)
            relay(k)

        def collect(k):
            zz = order[k]
            arrived(("y", run, k), y_rx.at[run, :, zz])
            first = own[0, zz] + y_rx[run, 2, zz].astype(F32) + y_rx[run, 1, zz].astype(F32)
            second = own[1, zz] + y_rx[run, 3, zz].astype(F32) + y_rx[run, 0, zz].astype(F32)
            if k == 0:
                arrived(("relay", run, 0), relay_rx.at[run, :, zo])
                first = first + relay_rx[run, 0, zo].astype(F32)
                second = second + relay_rx[run, 1, zo].astype(F32)
            return first, second

        def z_send(kind, d, value):
            z_tx[run, kind, d] = value.astype(BF16)
            send(
                ("z", run, min(kind, 1), d if kind == 0 else 0),
                ("z", run),
                z_tx.at[run, kind, d],
                z_rx.at[run, kind, d],
                z_to[d],
            )

        first, second = collect(0)
        z_send(0, 0, first)
        z_send(0, 1, second)
        between(1)
        first, second = collect(1)
        z_send(1, 0, second)
        rows_f32[0] = first
        first, second = collect(2)
        z_send(1, 1, first)
        rows_f32[1] = second
        for d in range(2):
            arrived(("z", run, 0, d), z_rx.at[run, 0, d])
            z_send(2, d, rows_f32[d] + z_rx[run, 0, d].astype(F32))
        between(2)
        first, second = collect(3)
        arrived(("z", run, 1, 0), z_rx.at[run, 1:3])
        between(3)
        first = first + z_rx[run, 2, 0].astype(F32) + z_rx[run, 1, 1].astype(F32)
        second = second + z_rx[run, 2, 1].astype(F32) + z_rx[run, 1, 0].astype(F32)
        return [first, second]

    loads[3].wait()
    arrived("halo", wide_v.at[0:2])
    sums = summed_terms(0, wide_v, lambda step: stat_sum(0, step))
    norm = total_of(0, 0) / cells
    shift = total_of(0, 1) / cells / (norm + EPSILON)

    crossed, squares = [], []
    for j in range(2):
        v = v_rows[j]
        sigma = jnp.where(masks[j], energies[j] * v + scale * sums[j], 0.0)
        u = sigma - shift * v
        wide_u[2 + j, z, y] = u.astype(BF16)
        sigma_out[j] = sigma
        next_out[j] = u
        crossed.append(u * v)
        squares.append(u * u)

    def rows_send(group, source, j, zz, yy, to):
        part = wide_u.at[2 + j, zz, yy]
        send(group, source, part, part, to)

    strips = [z, zm, zp, zo]
    across = [y, ym, yp, yo]

    def rows_arrived(group, j, zz, yy):
        arrived(group, wide_u.at[2 + j, zz, yy])

    def z_forward(d):
        zz = (zm, zp)[d]
        rows_arrived(("gz", d, d), d, zz, y)
        rows_send(("gzf", d), "gz", d, zz, y, z_to[d])

    def y_far(k):
        for j in range(2):
            rows_send(("gyf", k, j), "gyf", j, strips[k], y, {"term_1": yo})

    def y_near(k, j):
        for d in (j, 1 - j):
            rows_send(("gy", k, d, j), "gy", j, strips[k], y, y_to[d])

    def y_forward(k):
        for d in range(2):
            rows_arrived(("gy", k, d, d), d, strips[k], (ym, yp)[d])
            rows_send(("gyf", k, d), "gyf", d, strips[k], (ym, yp)[d], y_to[d])

    def y_rest(k):
        for d in range(2):
            rows_arrived(("gy", k, d, 1 - d), 1 - d, strips[k], (ym, yp)[d])

    def y_last(k):
        for d in range(2):
            rows_arrived(("gyf", k, d), d, strips[k], yo)

    def halo_send(j, k, m, to):
        part = (strips[k], across[m])
        send("gh", "gh", wide_u.at[2 + j, *part], wide_u.at[1 - j, *part], to)

    def halo(k, m):
        halo_send(1, k, m, beside[1])
        if k < 3 or m == 0:
            halo_send(0, k, m, beside[0])
        else:

            @pl.when(core == 1)
            def _():
                halo_send(0, k, m, beside[0])

        if k == 3 and m == 0:

            @pl.when(core == 0)
            def _():
                for to in outer:
                    halo_send(0, k, m, to)

    for first in (True, False):
        for d in range(2):
            j = d if first else 1 - d
            rows_send(("gz", d, j), "gz", j, z, y, z_to[d])
    for j in range(2):
        y_near(0, j)
    y_far(0)
    halo(0, 0)
    stat_tx[1, 0, 0] = fold(jnp.stack(crossed))
    stat_tx[1, 0, 1] = fold(jnp.stack(squares))
    stat_send(1, 0)
    for d in range(2):
        z_forward(d)
        y_near(1 + d, d)
    stat_sum(1, 0)
    for d in range(2):
        rows_arrived(("gz", d, 1 - d), 1 - d, (zm, zp)[d], y)
        y_near(1 + d, 1 - d)
    halo(1, 0)
    halo(2, 0)
    for d in range(2):
        rows_arrived(("gy", 0, d, d), d, z, (ym, yp)[d])
    y_rest(0)
    halo(0, 1)
    halo(0, 2)
    y_last(0)
    halo(0, 3)
    y_forward(1)
    stat_sum(1, 1)
    y_forward(2)
    for d in range(2):
        rows_arrived(("gzf", d), d, zo, y)
    y_far(3)
    for j in range(2):
        y_near(3, j)
    halo(3, 0)
    stat_sum(1, 2)
    for k in (1, 2):
        y_rest(k)
        halo(k, 1)
        halo(k, 2)
    for k in (1, 2):
        y_last(k)
        halo(k, 3)
    for d in range(2):
        rows_arrived(("gy", 3, d, d), d, zo, (ym, yp)[d])
    y_rest(3)
    halo(3, 1)
    halo(3, 2)
    stat_sum(1, 3)
    y_last(3)
    halo(3, 3)
    arrived("gh", wide_u.at[0:2])

    sums = summed_terms(1, wide_u, lambda step: stat_sum(1, step + 4))

    cross, square = total_of(1, 0) / cells, total_of(1, 1) / cells
    gap = (cross - shift * EPSILON) / (norm + EPSILON)
    residual_sq = square - 2.0 * gap * cross + gap * gap * norm
    inverse = 1.0 / jnp.sqrt(jnp.maximum(residual_sq, 0.0) + EPSILON)
    for j in range(2):
        u, sigma = next_out[j], sigma_out[j]
        next_out[j] = inverse * (u - gap * v_rows[j])
        applied = jnp.where(masks[j], energies[j] * u + scale * sums[j], 0.0)
        sigma_out[j] = inverse * (applied - gap * sigma)

    sent("halo", wide_v.at[2:4])
    for run in range(2):
        sent(("relay", run), opp_tx.at[run])
        sent(("y", run), y_tx.at[run])
        sent(("z", run), z_tx.at[run])
        sent(("stat", run), stat_tx.at[run, 0 : last_stage[run]])
    sent("gz", z_tx.at[0])
    sent("gy", y_tx.at[0])
    sent("gyf", opp_tx.at[0])
    sent("gh", wide_u.at[2:4])


def on_device(
    dims, lanczos_vector, left_block, right_block, left_energy, right_energy, sector_shifts, sector_sizes
):
    n_z, n_y = dims[3:]
    sectors, block, width = lanczos_vector.shape
    terms = left_block.shape[1]
    span = block // (n_z * n_y)
    strips = (n_z, n_y, span)
    out = pltpu.VMEM((sectors, span, width), F32)
    exchange = [pltpu.VMEM((2, parts, n_z, span, width), BF16) for parts in (2, 2, 4, 4)]
    vmem = pl.BlockSpec(memory_space=pltpu.VMEM)
    hbm = pl.BlockSpec(memory_space=pl.ANY)
    return pl.pallas_call(
        functools.partial(kernel, dims),
        out_shape=(out, out),
        in_specs=[hbm] * 7,
        out_specs=(vmem, vmem),
        scratch_shapes=[
            pltpu.SMEM((terms,), jnp.int32),
            pltpu.SMEM((sectors,), jnp.int32),
            pltpu.VMEM((sectors, block), F32),
            pltpu.VMEM((sectors, width), F32),
            pltpu.VMEM((sectors, n_z * n_y, span, width), F32),
            pltpu.VMEM((sectors, span, width), F32),
            pltpu.VMEM((sectors, terms, *strips, width), BF16),
            pltpu.VMEM((sectors, terms, block, width), BF16),
            pltpu.VMEM((5, *strips, width), BF16),
            pltpu.VMEM((5, *strips, width), BF16),
            *exchange,
            pltpu.VMEM((2, n_z, span, width), F32),
            pltpu.VMEM((2, n_z, span, width), F32),
            pltpu.VMEM((2, 3, 2, span, width), BF16),
            pltpu.VMEM((2, 3, 2, span, width), BF16),
            pltpu.VMEM((2, span, width), F32),
            pltpu.VMEM((sectors, n_z * span, terms * width), BF16),
            pltpu.VMEM((sectors, terms * width, block), BF16),
            pltpu.VMEM((2, 9, 2, 8, 128), F32),
            pltpu.VMEM((2, 8, 2, 8, 128), F32),
            pltpu.SemaphoreType.DMA((9,)),
            pltpu.SemaphoreType.DMA((SOURCES,)),
            pltpu.SemaphoreType.DMA((GROUPS,)),
        ],
        compiler_params=pltpu.CompilerParams(collective_id=0, has_side_effects=True),
        name="davidson_step",
    )(
        sector_shifts,
        sector_sizes,
        left_energy,
        right_energy,
        lanczos_vector.reshape(sectors, n_z * n_y, span, width),
        left_block.reshape(sectors, terms, *strips, width),
        right_block,
    )


def solution(mesh):
    dims = (2, 4, 2, 4, 4)
    finer = Mesh(mesh.devices.reshape(*dims), (*SECTOR, *TERM))
    return jax.shard_map(
        functools.partial(on_device, dims),
        mesh=finer,
        in_specs=(
            P(SECTOR, None, None),
            P(SECTOR, TERM, None, None),
            P(SECTOR, TERM, None, None),
            P(SECTOR, None),
            P(SECTOR, None),
            P(TERM),
            P(SECTOR),
        ),
        out_specs=(P(SECTOR, TERM, None), P(SECTOR, TERM, None)),
        check_vma=False,
    )
```

```python
import functools

import jax
import jax.numpy as jnp
from jax import lax
from jax.experimental import pallas as pl
from jax.experimental.pallas import tpu as pltpu
from jax.sharding import Mesh
from jax.sharding import PartitionSpec as P

TERM = ("term_0", "term_1")
SECTOR = ("sector_0", "sector_1", "sector_2")
MESH = pl.DeviceIdType.MESH
F32, BF16 = jnp.float32, jnp.bfloat16
EPSILON = 1e-06
GROUPS, SOURCES = 66, 12


def fold(values):
    total = None
    for j in range(values.shape[0]):
        for r in range(0, values.shape[1], 8):
            for c in range(0, values.shape[2], 128):
                piece = values[j, r : r + 8, c : c + 128]
                total = piece if total is None else total + piece
    return total


def kernel(
    dims,
    shifts_hbm,
    sizes_hbm,
    left_energy_hbm,
    right_energy_hbm,
    v_hbm,
    left_hbm,
    right_hbm,
    next_out,
    sigma_out,
    shifts,
    sizes,
    left_energy,
    right_energy,
    v_full,
    v_rows,
    left,
    right,
    wide_v,
    wide_u,
    opp_tx,
    relay_rx,
    y_tx,
    y_rx,
    near,
    own,
    z_tx,
    z_rx,
    rows_f32,
    mixed,
    turned,
    stat_tx,
    stat_rx,
    load_sem,
    send_sem,
    recv_sem,
):
    n_lo, n_x, n_core, n_z, n_y = dims
    terms = left.shape[1]
    span, width = v_rows.shape[1], v_rows.shape[2]
    n_sec = n_lo * n_x * n_core
    block = n_z * n_y * span
    scale = float(terms * n_z * n_y) ** (-0.5)
    cells = float(2 * n_sec * block * width)

    lo, x, core = [lax.axis_index(a) for a in SECTOR]
    z, y = [lax.axis_index(a) for a in TERM]
    sec = (lo * n_x + x) * n_core + core
    rank = z * n_y + y
    zs = [lax.rem(z + k, n_z) for k in range(n_z)]
    ys = [lax.rem(y + k, n_y) for k in range(n_y)]
    zp, zo, zm = zs[1], zs[2], zs[3]
    yp, yo, ym = ys[1], ys[2], ys[3]
    y_next = [yp, ym]
    y_to = [{"term_1": yp}, {"term_1": ym}]
    z_to = [{"term_0": zp}, {"term_0": zm}]

    def sector_device(s):
        s = lax.rem(s, n_sec)
        return {
            "sector_0": s // (n_x * n_core),
            "sector_1": lax.rem(s // n_core, n_x),
            "sector_2": lax.rem(s, n_core),
        }

    beside = [sector_device(sec + n_sec - 1), sector_device(sec + 1)]
    first_one, last_one = sec == 0, sec == n_sec - 1
    at_end = first_one | last_one


    def pair(i):
        return i + 1 - 2 * lax.rem(i, 2)

    stages = [
        {"sector_1": pair(x)},
        {"sector_1": n_x - 1 - x},
        {"sector_0": 1 - lo},
        {"sector_2": 1 - core},
        {"term_0": pair(z)},
        {"term_0": n_z - 1 - z},
        {"term_1": pair(y)},
        {"term_1": n_y - 1 - y},
    ]
    last_stage = [4, 8]

    barrier = pltpu.get_barrier_semaphore()
    peers = [*beside, *y_to, {"term_1": yo}, *z_to, *stages[:3]]
    for peer in peers:
        pl.semaphore_signal(barrier, inc=1, device_id=peer, device_id_type=MESH)

    loads = [pltpu.make_async_copy(v_hbm.at[:, rank], v_rows, load_sem.at[0])]
    for j in range(2):
        loads.append(pltpu.make_async_copy(v_hbm.at[j], v_full.at[j], load_sem.at[1 + j]))
    small = [
        (sizes_hbm, sizes),
        (shifts_hbm, shifts),
        (left_energy_hbm, left_energy),
        (right_energy_hbm, right_energy),
    ]
    small = [pltpu.make_async_copy(a, b, load_sem.at[5 + i]) for i, (a, b) in enumerate(small)]
    for load in small:
        load.start()
    loads.append(pltpu.make_async_copy(left_hbm, left, load_sem.at[3]))
    loads.append(pltpu.make_async_copy(right_hbm, right, load_sem.at[4]))
    for load in loads:
        load.start()

    groups, sources = {}, {}

    def send(group, source, src, dst, to):
        pltpu.make_async_remote_copy(
            src_ref=src,
            dst_ref=dst,
            send_sem=send_sem.at[sources.setdefault(source, len(sources))],
            recv_sem=recv_sem.at[groups.setdefault(group, len(groups))],
            device_id=to,
            device_id_type=MESH,
        ).start()

    def arrived(group, like):
        pltpu.make_async_copy(like, like, recv_sem.at[groups[group]]).wait()

    def end_or_both(wait, key, like):
        pl.when(at_end)(lambda: wait(key, like.at[0:1]))
        pl.when(jnp.logical_not(at_end))(lambda: wait(key, like))

    def sent(source, like):
        pltpu.make_async_copy(like, like, send_sem.at[sources[source]]).wait()

    def stat_send(run, stage):
        send(
            ("stat", run, stage),
            ("stat", run),
            stat_tx.at[run, stage],
            stat_rx.at[run, stage],
            stages[stage],
        )

    def stat_sum(run, stage):
        arrived(("stat", run, stage), stat_rx.at[run, stage])
        stat_tx[run, stage + 1] = stat_tx[run, stage] + stat_rx[run, stage]
        if stage + 1 < last_stage[run]:
            stat_send(run, stage + 1)

    def total_of(run, which):
        return jnp.sum(stat_tx[run, last_stage[run], which], keepdims=True)

    for load in small:
        load.wait()
    row = lax.broadcasted_iota(jnp.int32, (span, width), 0) + rank * span
    col = lax.broadcasted_iota(jnp.int32, (span, width), 1)
    masks, energies = [], []
    for j in range(2):
        masks.append((row < sizes[j]) & (col < sizes[j]))
        le = jnp.where(row == col, left_energy[j : j + 1, :], 0.0)
        energies.append(jnp.sum(le, axis=1, keepdims=True) + right_energy[j : j + 1, :])

    zero = jnp.zeros((n_y, span, width), BF16)
    for k in range(n_z):
        wide_v[4, k] = zero
        wide_u[4, k] = zero
    for slot, here in enumerate((first_one, last_one)):

        @pl.when(here)
        def _():
            for k in range(n_z):
                wide_v[slot, k] = zero
                wide_u[slot, k] = zero

    pl.semaphore_wait(barrier, len(peers))
    for j in range(2):
        loads[1 + j].wait()
        for k in range(n_z * n_y):
            r = lax.broadcasted_iota(jnp.int32, (span, width), 0) + k * span
            keep = (r < sizes[j]) & (col < sizes[j])
            wide_v[2 + j, k // n_y, k % n_y] = jnp.where(keep, v_full[j, k], 0.0).astype(BF16)

        @pl.when(jnp.logical_not((first_one, last_one)[j]))
        def _():
            send("halo", "halo", wide_v.at[2 + j], wide_v.at[1 - j], beside[j])


    eye = (
        lax.broadcasted_iota(jnp.int32, (span, 128), 0)
        - lax.broadcasted_iota(jnp.int32, (span, 128), 1)
    )
    squares = jnp.zeros((8, 128), F32)
    weighted = jnp.zeros((8, 128), F32)
    for j in range(2):
        for k in range(n_z * n_y):
            at = k * span // 128 * 128
            le = jnp.where(eye == at - k * span, left_energy[j : j + 1, at : at + 128], 0.0)
            energy = jnp.sum(le, axis=1, keepdims=True) + right_energy[j : j + 1, :]
            r = lax.broadcasted_iota(jnp.int32, (span, width), 0) + k * span
            keep = (r < sizes[j]) & (col < sizes[j])
            v = jnp.where(keep, v_full[j, k], 0.0)
            squares = squares + fold((v * v)[None])
            weighted = weighted + fold((v * v * energy)[None])
    stat_tx[0, 0, 0] = squares
    stat_tx[0, 0, 1] = weighted
    stat_send(0, 0)
    loads[0].wait()
    for j in range(2):
        v_rows[j] = jnp.where(masks[j], v_rows[j], 0.0)

    loads[4].wait()
    half = 256
    ones = lax.broadcasted_iota(jnp.int32, (half, half), 0) == lax.broadcasted_iota(
        jnp.int32, (half, half), 1
    )
    ones = ones.astype(F32).astype(BF16)
    for j in range(2):
        for t in range(terms):
            for a in range(0, block, half):
                for b in range(0, width, half):
                    turned[j, t * width + b : t * width + b + half, a : a + half] = lax.dot_general(
                        ones,
                        right[j, t, a : a + half, b : b + half],
                        (((1,), (1,)), ((), ())),
                        preferred_element_type=F32,
                    ).astype(BF16)

    slots = []
    for j in range(2):
        for t in range(terms):
            p = 1 + j + shifts[t]
            outside = ((sec == 0) & (p == 0)) | ((sec == n_sec - 1) & (p == 3))
            slots.append(jnp.where(outside, 4, jnp.where(p == 0, 0, jnp.where(p == 3, 1, p + 1))))

    def chunk(vector, j, yy):
        for t in range(terms):
            rows = left[j, t, :, yy].reshape(n_z * span, block)
            paired = vector[slots[j * terms + t]].reshape(block, width)
            mixed[j, :, t * width : (t + 1) * width] = jnp.dot(
                rows, paired, preferred_element_type=F32
            ).astype(BF16)
        total = jnp.dot(mixed[j], turned[j], preferred_element_type=F32)
        return total.reshape(n_z, span, block)

    def summed_terms(run, vector, between):
        order = [zo, zp, zm, z]
        for d in range(2):
            opp_tx[run, d] = chunk(vector, d, yo).astype(BF16)
            for k, zz in enumerate(order):
                send(
                    ("relay", run, k),
                    ("relay", run),
                    opp_tx.at[run, d, zz],
                    relay_rx.at[run, d, zz],
                    y_to[d] if k else {"term_1": yo},
                )

        def y_send(k, kind, d):
            part = 2 * kind + d
            send(
                ("y", run, k),
                ("y", run),
                y_tx.at[run, part, order[k]],
                y_rx.at[run, part, order[k]],
                y_to[d],
            )

        def relay(k):
            zz = order[k]
            arrived(("relay", run, k), relay_rx.at[run, :, zz])
            for d in range(2):
                y_tx[run, 2 + d, zz] = (near[d, zz] + relay_rx[run, d, zz].astype(F32)).astype(BF16)
                y_send(k, 1, d)

        for d in range(2):
            y_tx[run, d] = chunk(vector, 1 - d, y_next[d]).astype(BF16)
            y_send(0, 0, d)
        for d in range(2):
            near[d] = chunk(vector, d, y_next[d])
            y_tx[run, 2 + d, zo] = near[d, zo].astype(BF16)
            y_send(0, 1, d)
        between(0)
        for k in range(1, n_z):
            for d in range(2):
                y_send(k, 0, d)
            if k < 3:
                own[k - 1] = chunk(vector, k - 1, y)
            relay(k)

        def collect(k):
            zz = order[k]
            arrived(("y", run, k), y_rx.at[run, :, zz])
            first = own[0, zz] + y_rx[run, 2, zz].astype(F32) + y_rx[run, 1, zz].astype(F32)
            second = own[1, zz] + y_rx[run, 3, zz].astype(F32) + y_rx[run, 0, zz].astype(F32)
            if k == 0:
                arrived(("relay", run, 0), relay_rx.at[run, :, zo])
                first = first + relay_rx[run, 0, zo].astype(F32)
                second = second + relay_rx[run, 1, zo].astype(F32)
            return first, second

        def z_send(kind, d, value):
            z_tx[run, kind, d] = value.astype(BF16)
            send(
                ("z", run, min(kind, 1), d if kind == 0 else 0),
                ("z", run),
                z_tx.at[run, kind, d],
                z_rx.at[run, kind, d],
                z_to[d],
            )

        first, second = collect(0)
        z_send(0, 0, first)
        z_send(0, 1, second)
        between(1)
        first, second = collect(1)
        z_send(1, 0, second)
        rows_f32[0] = first
        first, second = collect(2)
        z_send(1, 1, first)
        rows_f32[1] = second
        for d in range(2):
            arrived(("z", run, 0, d), z_rx.at[run, 0, d])
            z_send(2, d, rows_f32[d] + z_rx[run, 0, d].astype(F32))
        between(2)
        first, second = collect(3)
        arrived(("z", run, 1, 0), z_rx.at[run, 1:3])
        between(3)
        first = first + z_rx[run, 2, 0].astype(F32) + z_rx[run, 1, 1].astype(F32)
        second = second + z_rx[run, 2, 1].astype(F32) + z_rx[run, 1, 0].astype(F32)
        return [first, second]

    loads[3].wait()
    end_or_both(arrived, "halo", wide_v.at[0:2])
    sums = summed_terms(0, wide_v, lambda step: stat_sum(0, step))
    norm = total_of(0, 0) / cells
    shift = total_of(0, 1) / cells / (norm + EPSILON)

    crossed, squares = [], []
    for j in range(2):
        v = v_rows[j]
        sigma = jnp.where(masks[j], energies[j] * v + scale * sums[j], 0.0)
        u = sigma - shift * v
        wide_u[2 + j, z, y] = u.astype(BF16)
        sigma_out[j] = sigma
        next_out[j] = u
        crossed.append(u * v)
        squares.append(u * u)

    def rows_send(group, source, j, zz, yy, to):
        part = wide_u.at[2 + j, zz, yy]
        send(group, source, part, part, to)

    strips = [z, zm, zp, zo]
    across = [y, ym, yp, yo]

    def rows_arrived(group, j, zz, yy):
        arrived(group, wide_u.at[2 + j, zz, yy])

    def z_forward(d):
        zz = (zm, zp)[d]
        rows_arrived(("gz", d, d), d, zz, y)
        rows_send(("gzf", d), "gz", d, zz, y, z_to[d])

    def y_own(k):
        for first in (True, False):
            for d in range(2):
                j = d if first else 1 - d
                rows_send(("gy", k, d, j), "gy", j, strips[k], y, y_to[d])

    def y_forward(k):
        for d in range(2):
            rows_arrived(("gy", k, d, d), d, strips[k], (ym, yp)[d])
            rows_send(("gyf", k, d), "gy", d, strips[k], (ym, yp)[d], y_to[d])

    def y_rest(k):
        for d in range(2):
            rows_arrived(("gy", k, d, 1 - d), 1 - d, strips[k], (ym, yp)[d])

    def y_last(k):
        for d in range(2):
            rows_arrived(("gyf", k, d), d, strips[k], yo)

    def halo(k, m):
        for j in range(2):
            part = (strips[k], across[m])

            @pl.when(jnp.logical_not((first_one, last_one)[j]))
            def _():
                send("gh", "gh", wide_u.at[2 + j, *part], wide_u.at[1 - j, *part], beside[j])


    for first in (True, False):
        for d in range(2):
            j = d if first else 1 - d
            rows_send(("gz", d, j), "gz", j, z, y, z_to[d])
    y_own(0)
    halo(0, 0)
    stat_tx[1, 0, 0] = fold(jnp.stack(crossed))
    stat_tx[1, 0, 1] = fold(jnp.stack(squares))
    stat_send(1, 0)
    y_forward(0)
    y_rest(0)
    halo(0, 1)
    halo(0, 2)
    for d in range(2):
        z_forward(d)
    for d in range(2):
        rows_arrived(("gz", d, 1 - d), 1 - d, (zm, zp)[d], y)
    y_own(1)
    y_own(2)
    halo(1, 0)
    halo(2, 0)
    stat_sum(1, 0)
    y_last(0)
    halo(0, 3)
    for d in range(2):
        rows_arrived(("gzf", d), d, zo, y)
    for j in range(2):
        rows_send(("gyf", 3, j), "gy", j, zo, y, {"term_1": yo})
    y_own(3)
    halo(3, 0)
    stat_sum(1, 1)
    for k in (1, 2):
        y_forward(k)
        y_rest(k)
        halo(k, 1)
        halo(k, 2)
    for d in range(2):
        rows_arrived(("gy", 3, d, d), d, zo, (ym, yp)[d])
    y_rest(3)
    halo(3, 1)
    halo(3, 2)
    stat_sum(1, 2)
    for k in (1, 2, 3):
        y_last(k)
        halo(k, 3)
    stat_sum(1, 3)
    end_or_both(arrived, "gh", wide_u.at[0:2])

    sums = summed_terms(1, wide_u, lambda step: stat_sum(1, step + 4))

    cross, square = total_of(1, 0) / cells, total_of(1, 1) / cells
    gap = (cross - shift * EPSILON) / (norm + EPSILON)
    residual_sq = square - 2.0 * gap * cross + gap * gap * norm
    inverse = 1.0 / jnp.sqrt(jnp.maximum(residual_sq, 0.0) + EPSILON)
    for j in range(2):
        u, sigma = next_out[j], sigma_out[j]
        next_out[j] = inverse * (u - gap * v_rows[j])
        applied = jnp.where(masks[j], energies[j] * u + scale * sums[j], 0.0)
        sigma_out[j] = inverse * (applied - gap * sigma)

    end_or_both(sent, "halo", wide_v.at[2:4])
    for run in range(2):
        sent(("relay", run), opp_tx.at[run])
        sent(("y", run), y_tx.at[run])
        sent(("z", run), z_tx.at[run])
        sent(("stat", run), stat_tx.at[run, 0 : last_stage[run]])
    sent("gz", z_tx.at[0])
    sent("gy", left.at[0, 0:2, 0:3])
    end_or_both(sent, "gh", wide_u.at[2:4])


def write_out(next_in, sigma_in, next_out, sigma_out, sem):
    pairs = ((next_in, next_out), (sigma_in, sigma_out))
    copies = [pltpu.make_async_copy(a, b, sem.at[i]) for i, (a, b) in enumerate(pairs)]
    for copy in copies:
        copy.start()
    for copy in copies:
        copy.wait()


def on_device(
    dims, lanczos_vector, left_block, right_block, left_energy, right_energy, sector_shifts, sector_sizes
):
    n_z, n_y = dims[3:]
    sectors, block, width = lanczos_vector.shape
    terms = left_block.shape[1]
    span = block // (n_z * n_y)
    strips = (n_z, n_y, span)
    out = pltpu.VMEM((sectors, span, width), F32)
    exchange = [pltpu.VMEM((2, parts, n_z, span, width), BF16) for parts in (2, 2, 4, 4)]
    vmem = pl.BlockSpec(memory_space=pltpu.VMEM)
    hbm = pl.BlockSpec(memory_space=pl.ANY)
    results = pl.pallas_call(
        functools.partial(kernel, dims),
        out_shape=(out, out),
        in_specs=[hbm] * 7,
        out_specs=(vmem, vmem),
        scratch_shapes=[
            pltpu.SMEM((terms,), jnp.int32),
            pltpu.SMEM((sectors,), jnp.int32),
            pltpu.VMEM((sectors, block), F32),
            pltpu.VMEM((sectors, width), F32),
            pltpu.VMEM((sectors, n_z * n_y, span, width), F32),
            pltpu.VMEM((sectors, span, width), F32),
            pltpu.VMEM((sectors, terms, *strips, width), BF16),
            pltpu.VMEM((sectors, terms, block, width), BF16),
            pltpu.VMEM((5, *strips, width), BF16),
            pltpu.VMEM((5, *strips, width), BF16),
            *exchange,
            pltpu.VMEM((2, n_z, span, width), F32),
            pltpu.VMEM((2, n_z, span, width), F32),
            pltpu.VMEM((2, 3, 2, span, width), BF16),
            pltpu.VMEM((2, 3, 2, span, width), BF16),
            pltpu.VMEM((2, span, width), F32),
            pltpu.VMEM((sectors, n_z * span, terms * width), BF16),
            pltpu.VMEM((sectors, terms * width, block), BF16),
            pltpu.VMEM((2, 9, 2, 8, 128), F32),
            pltpu.VMEM((2, 8, 2, 8, 128), F32),
            pltpu.SemaphoreType.DMA((9,)),
            pltpu.SemaphoreType.DMA((SOURCES,)),
            pltpu.SemaphoreType.DMA((GROUPS,)),
        ],
        compiler_params=pltpu.CompilerParams(collective_id=0, has_side_effects=True),
        name="davidson_step",
    )(
        sector_shifts,
        sector_sizes,
        left_energy,
        right_energy,
        lanczos_vector.reshape(sectors, n_z * n_y, span, width),
        left_block.reshape(sectors, terms, *strips, width),
        right_block,
    )
    whole = jax.ShapeDtypeStruct((sectors, span, width), F32)
    return pl.pallas_call(
        write_out,
        out_shape=(whole, whole),
        in_specs=[hbm, hbm],
        out_specs=(hbm, hbm),
        scratch_shapes=[pltpu.SemaphoreType.DMA((2,))],
        compiler_params=pltpu.CompilerParams(vmem_limit_bytes=1 << 20),
        name="write_out",
    )(*results)


def solution(mesh):
    dims = (2, 4, 2, 4, 4)
    finer = Mesh(mesh.devices.reshape(*dims), (*SECTOR, *TERM))
    return jax.shard_map(
        functools.partial(on_device, dims),
        mesh=finer,
        in_specs=(
            P(SECTOR, None, None),
            P(SECTOR, TERM, None, None),
            P(SECTOR, TERM, None, None),
            P(SECTOR, None),
            P(SECTOR, None),
            P(TERM),
            P(SECTOR),
        ),
        out_specs=(P(SECTOR, TERM, None), P(SECTOR, TERM, None)),
        check_vma=False,
    )
```

```python
import functools

import jax
import jax.numpy as jnp
from jax import lax
from jax.experimental import pallas as pl
from jax.experimental.pallas import tpu as pltpu
from jax.sharding import Mesh
from jax.sharding import PartitionSpec as P

TERM = ("term_0", "term_1")
SECTOR = ("sector_0", "sector_1", "sector_2")
MESH = pl.DeviceIdType.MESH
F32, BF16 = jnp.float32, jnp.bfloat16
EPSILON = 1e-06
GROUPS, SOURCES = 66, 12


def fold(values):
    total = None
    for j in range(values.shape[0]):
        for r in range(0, values.shape[1], 8):
            for c in range(0, values.shape[2], 128):
                piece = values[j, r : r + 8, c : c + 128]
                total = piece if total is None else total + piece
    return total


def kernel(
    dims,
    shifts_hbm,
    sizes_hbm,
    left_energy_hbm,
    right_energy_hbm,
    v_hbm,
    left_hbm,
    right_hbm,
    next_out,
    sigma_out,
    shifts,
    sizes,
    left_energy,
    right_energy,
    v_full,
    v_rows,
    left,
    right,
    wide_v,
    wide_u,
    opp_tx,
    relay_rx,
    y_tx,
    y_rx,
    near,
    own,
    z_tx,
    z_rx,
    rows_f32,
    mixed,
    turned,
    stat_tx,
    stat_rx,
    load_sem,
    send_sem,
    recv_sem,
):
    n_lo, n_x, n_core, n_z, n_y = dims
    terms = left.shape[1]
    span, width = v_rows.shape[1], v_rows.shape[2]
    n_sec = n_lo * n_x * n_core
    block = n_z * n_y * span
    scale = float(terms * n_z * n_y) ** (-0.5)
    cells = float(2 * n_sec * block * width)

    lo, x, core = [lax.axis_index(a) for a in SECTOR]
    z, y = [lax.axis_index(a) for a in TERM]
    sec = (lo * n_x + x) * n_core + core
    rank = z * n_y + y
    zs = [lax.rem(z + k, n_z) for k in range(n_z)]
    ys = [lax.rem(y + k, n_y) for k in range(n_y)]
    zp, zo, zm = zs[1], zs[2], zs[3]
    yp, yo, ym = ys[1], ys[2], ys[3]
    y_next = [yp, ym]
    y_to = [{"term_1": yp}, {"term_1": ym}]
    z_to = [{"term_0": zp}, {"term_0": zm}]

    def sector_device(s):
        s = lax.rem(s, n_sec)
        return {
            "sector_0": s // (n_x * n_core),
            "sector_1": lax.rem(s // n_core, n_x),
            "sector_2": lax.rem(s, n_core),
        }

    beside = [sector_device(sec + n_sec - 1), sector_device(sec + 1)]
    first_one, last_one = sec == 0, sec == n_sec - 1
    at_end = first_one | last_one


    def pair(i):
        return i + 1 - 2 * lax.rem(i, 2)

    stages = [
        {"sector_1": pair(x)},
        {"sector_1": n_x - 1 - x},
        {"sector_0": 1 - lo},
        {"sector_2": 1 - core},
        {"term_0": pair(z)},
        {"term_0": n_z - 1 - z},
        {"term_1": pair(y)},
        {"term_1": n_y - 1 - y},
    ]
    last_stage = [4, 8]

    barrier = pltpu.get_barrier_semaphore()
    peers = [*beside, *y_to, {"term_1": yo}, *z_to, *stages[:3]]
    for peer in peers:
        pl.semaphore_signal(barrier, inc=1, device_id=peer, device_id_type=MESH)

    loads = [pltpu.make_async_copy(v_hbm.at[:, rank], v_rows, load_sem.at[0])]
    for j in range(2):
        loads.append(pltpu.make_async_copy(v_hbm.at[j], v_full.at[j], load_sem.at[1 + j]))
    small = [
        (sizes_hbm, sizes),
        (shifts_hbm, shifts),
        (left_energy_hbm, left_energy),
        (right_energy_hbm, right_energy),
    ]
    small = [pltpu.make_async_copy(a, b, load_sem.at[5 + i]) for i, (a, b) in enumerate(small)]
    for load in small:
        load.start()
    loads.append(pltpu.make_async_copy(left_hbm, left, load_sem.at[3]))
    loads.append(pltpu.make_async_copy(right_hbm, right, load_sem.at[4]))
    for load in loads:
        load.start()

    groups, sources = {}, {}

    def send(group, source, src, dst, to):
        pltpu.make_async_remote_copy(
            src_ref=src,
            dst_ref=dst,
            send_sem=send_sem.at[sources.setdefault(source, len(sources))],
            recv_sem=recv_sem.at[groups.setdefault(group, len(groups))],
            device_id=to,
            device_id_type=MESH,
        ).start()

    def arrived(group, like):
        pltpu.make_async_copy(like, like, recv_sem.at[groups[group]]).wait()

    def end_or_both(wait, key, like):
        pl.when(at_end)(lambda: wait(key, like.at[0:1]))
        pl.when(jnp.logical_not(at_end))(lambda: wait(key, like))

    def sent(source, like):
        pltpu.make_async_copy(like, like, send_sem.at[sources[source]]).wait()

    def stat_send(run, stage):
        send(
            ("stat", run, stage),
            ("stat", run),
            stat_tx.at[run, stage],
            stat_rx.at[run, stage],
            stages[stage],
        )

    def stat_sum(run, stage):
        arrived(("stat", run, stage), stat_rx.at[run, stage])
        stat_tx[run, stage + 1] = stat_tx[run, stage] + stat_rx[run, stage]
        if stage + 1 < last_stage[run]:
            stat_send(run, stage + 1)

    def total_of(run, which):
        return jnp.sum(stat_tx[run, last_stage[run], which], keepdims=True)

    for load in small:
        load.wait()
    row = lax.broadcasted_iota(jnp.int32, (span, width), 0) + rank * span
    col = lax.broadcasted_iota(jnp.int32, (span, width), 1)
    masks, energies = [], []
    for j in range(2):
        masks.append((row < sizes[j]) & (col < sizes[j]))
        le = jnp.where(row == col, left_energy[j : j + 1, :], 0.0)
        energies.append(jnp.sum(le, axis=1, keepdims=True) + right_energy[j : j + 1, :])

    zero = jnp.zeros((n_y, span, width), BF16)
    for k in range(n_z):
        wide_v[4, k] = zero
        wide_u[4, k] = zero
    for slot, here in enumerate((first_one, last_one)):

        @pl.when(here)
        def _():
            for k in range(n_z):
                wide_v[slot, k] = zero
                wide_u[slot, k] = zero

    pl.semaphore_wait(barrier, len(peers))
    for j in range(2):
        loads[1 + j].wait()
        for k in range(n_z * n_y):
            r = lax.broadcasted_iota(jnp.int32, (span, width), 0) + k * span
            keep = (r < sizes[j]) & (col < sizes[j])
            wide_v[2 + j, k // n_y, k % n_y] = jnp.where(keep, v_full[j, k], 0.0).astype(BF16)

        @pl.when(jnp.logical_not((first_one, last_one)[j]))
        def _():
            send("halo", "halo", wide_v.at[2 + j], wide_v.at[1 - j], beside[j])


    eye = (
        lax.broadcasted_iota(jnp.int32, (span, 128), 0)
        - lax.broadcasted_iota(jnp.int32, (span, 128), 1)
    )
    squares = jnp.zeros((8, 128), F32)
    weighted = jnp.zeros((8, 128), F32)
    for j in range(2):
        for k in range(n_z * n_y):
            at = k * span // 128 * 128
            le = jnp.where(eye == at - k * span, left_energy[j : j + 1, at : at + 128], 0.0)
            energy = jnp.sum(le, axis=1, keepdims=True) + right_energy[j : j + 1, :]
            r = lax.broadcasted_iota(jnp.int32, (span, width), 0) + k * span
            keep = (r < sizes[j]) & (col < sizes[j])
            v = jnp.where(keep, v_full[j, k], 0.0)
            squares = squares + fold((v * v)[None])
            weighted = weighted + fold((v * v * energy)[None])
    stat_tx[0, 0, 0] = squares
    stat_tx[0, 0, 1] = weighted
    stat_send(0, 0)
    loads[0].wait()
    for j in range(2):
        v_rows[j] = jnp.where(masks[j], v_rows[j], 0.0)

    loads[4].wait()
    half = 256
    ones = lax.broadcasted_iota(jnp.int32, (half, half), 0) == lax.broadcasted_iota(
        jnp.int32, (half, half), 1
    )
    ones = ones.astype(F32).astype(BF16)
    for j in range(2):
        for t in range(terms):
            for a in range(0, block, half):
                for b in range(0, width, half):
                    turned[j, t * width + b : t * width + b + half, a : a + half] = lax.dot_general(
                        ones,
                        right[j, t, a : a + half, b : b + half],
                        (((1,), (1,)), ((), ())),
                        preferred_element_type=F32,
                    ).astype(BF16)

    slots = []
    for j in range(2):
        for t in range(terms):
            p = 1 + j + shifts[t]
            outside = ((sec == 0) & (p == 0)) | ((sec == n_sec - 1) & (p == 3))
            slots.append(jnp.where(outside, 4, jnp.where(p == 0, 0, jnp.where(p == 3, 1, p + 1))))

    def chunk(vector, j, yy):
        for t in range(terms):
            rows = left[j, t, :, yy].reshape(n_z * span, block)
            paired = vector[slots[j * terms + t]].reshape(block, width)
            mixed[j, :, t * width : (t + 1) * width] = jnp.dot(
                rows, paired, preferred_element_type=F32
            ).astype(BF16)
        total = jnp.dot(mixed[j], turned[j], preferred_element_type=F32)
        return total.reshape(n_z, span, block)

    def summed_terms(run, vector, between):
        order = [zo, zp, zm, z]
        for d in range(2):
            opp_tx[run, d] = chunk(vector, d, yo).astype(BF16)
            for k, zz in enumerate(order):
                send(
                    ("relay", run, k),
                    ("relay", run),
                    opp_tx.at[run, d, zz],
                    relay_rx.at[run, d, zz],
                    y_to[d] if k else {"term_1": yo},
                )

        def y_send(k, kind, d):
            part = 2 * kind + d
            send(
                ("y", run, k),
                ("y", run),
                y_tx.at[run, part, order[k]],
                y_rx.at[run, part, order[k]],
                y_to[d],
            )

        def relay(k):
            zz = order[k]
            arrived(("relay", run, k), relay_rx.at[run, :, zz])
            for d in range(2):
                y_tx[run, 2 + d, zz] = (near[d, zz] + relay_rx[run, d, zz].astype(F32)).astype(BF16)
                y_send(k, 1, d)

        for d in range(2):
            y_tx[run, d] = chunk(vector, 1 - d, y_next[d]).astype(BF16)
            y_send(0, 0, d)
        for d in range(2):
            near[d] = chunk(vector, d, y_next[d])
            y_tx[run, 2 + d, zo] = near[d, zo].astype(BF16)
            y_send(0, 1, d)
        between(0)
        for k in range(1, n_z):
            for d in range(2):
                y_send(k, 0, d)
            if k < 3:
                own[k - 1] = chunk(vector, k - 1, y)
            relay(k)

        def collect(k):
            zz = order[k]
            arrived(("y", run, k), y_rx.at[run, :, zz])
            first = own[0, zz] + y_rx[run, 2, zz].astype(F32) + y_rx[run, 1, zz].astype(F32)
            second = own[1, zz] + y_rx[run, 3, zz].astype(F32) + y_rx[run, 0, zz].astype(F32)
            if k == 0:
                arrived(("relay", run, 0), relay_rx.at[run, :, zo])
                first = first + relay_rx[run, 0, zo].astype(F32)
                second = second + relay_rx[run, 1, zo].astype(F32)
            return first, second

        def z_send(kind, d, value):
            z_tx[run, kind, d] = value.astype(BF16)
            send(
                ("z", run, min(kind, 1), d if kind == 0 else 0),
                ("z", run),
                z_tx.at[run, kind, d],
                z_rx.at[run, kind, d],
                z_to[d],
            )

        first, second = collect(0)
        z_send(0, 0, first)
        z_send(0, 1, second)
        between(1)
        first, second = collect(1)
        z_send(1, 0, second)
        rows_f32[0] = first
        first, second = collect(2)
        z_send(1, 1, first)
        rows_f32[1] = second
        for d in range(2):
            arrived(("z", run, 0, d), z_rx.at[run, 0, d])
            z_send(2, d, rows_f32[d] + z_rx[run, 0, d].astype(F32))
        between(2)
        first, second = collect(3)
        arrived(("z", run, 1, 0), z_rx.at[run, 1:3])
        between(3)
        first = first + z_rx[run, 2, 0].astype(F32) + z_rx[run, 1, 1].astype(F32)
        second = second + z_rx[run, 2, 1].astype(F32) + z_rx[run, 1, 0].astype(F32)
        return [first, second]

    loads[3].wait()
    end_or_both(arrived, "halo", wide_v.at[0:2])
    sums = summed_terms(0, wide_v, lambda step: stat_sum(0, step))
    norm = total_of(0, 0) / cells
    shift = total_of(0, 1) / cells / (norm + EPSILON)

    crossed, squares = [], []
    for j in range(2):
        v = v_rows[j]
        sigma = jnp.where(masks[j], energies[j] * v + scale * sums[j], 0.0)
        u = sigma - shift * v
        wide_u[2 + j, z, y] = u.astype(BF16)
        sigma_out[j] = sigma
        next_out[j] = u
        crossed.append(u * v)
        squares.append(u * u)

    def rows_send(group, source, j, zz, yy, to):
        part = wide_u.at[2 + j, zz, yy]
        send(group, source, part, part, to)

    strips = [z, zm, zp, zo]
    across = [y, ym, yp, yo]

    def rows_arrived(group, j, zz, yy):
        arrived(group, wide_u.at[2 + j, zz, yy])

    def z_forward(d):
        zz = (zm, zp)[d]
        rows_arrived(("gz", d, d), d, zz, y)
        rows_send(("gzf", d), "gz", d, zz, y, z_to[d])

    def y_own(k):
        for first in (True, False):
            for d in range(2):
                j = d if first else 1 - d
                rows_send(("gy", k, d, j), "gy", j, strips[k], y, y_to[d])

    def y_forward(k):
        for d in range(2):
            rows_arrived(("gy", k, d, d), d, strips[k], (ym, yp)[d])
            rows_send(("gyf", k, d), "gy", d, strips[k], (ym, yp)[d], y_to[d])

    def y_rest(k):
        for d in range(2):
            rows_arrived(("gy", k, d, 1 - d), 1 - d, strips[k], (ym, yp)[d])

    def y_last(k):
        for d in range(2):
            rows_arrived(("gyf", k, d), d, strips[k], yo)

    def halo(k, m):
        for j in range(2):
            part = (strips[k], across[m])

            @pl.when(jnp.logical_not((first_one, last_one)[j]))
            def _():
                send("gh", "gh", wide_u.at[2 + j, *part], wide_u.at[1 - j, *part], beside[j])


    for first in (True, False):
        for d in range(2):
            j = d if first else 1 - d
            rows_send(("gz", d, j), "gz", j, z, y, z_to[d])
    y_own(0)
    halo(0, 0)
    stat_tx[1, 0, 0] = fold(jnp.stack(crossed))
    stat_tx[1, 0, 1] = fold(jnp.stack(squares))
    stat_send(1, 0)
    y_forward(0)
    y_rest(0)
    halo(0, 1)
    halo(0, 2)
    for d in range(2):
        z_forward(d)
    for d in range(2):
        rows_arrived(("gz", d, 1 - d), 1 - d, (zm, zp)[d], y)
    y_own(1)
    y_own(2)
    halo(1, 0)
    halo(2, 0)
    stat_sum(1, 0)
    y_last(0)
    halo(0, 3)
    for j in range(2):
        rows_arrived(("gzf", j), j, zo, y)
        rows_send(("gyf", 3, j), "gy", j, zo, y, {"term_1": yo})
        for d in (j, 1 - j):
            rows_send(("gy", 3, d, j), "gy", j, zo, y, y_to[d])
    halo(3, 0)
    stat_sum(1, 1)
    for k in (1, 2):
        y_forward(k)
        y_rest(k)
        halo(k, 1)
        halo(k, 2)
    for d in range(2):
        rows_arrived(("gy", 3, d, d), d, zo, (ym, yp)[d])
    y_rest(3)
    halo(3, 1)
    halo(3, 2)
    stat_sum(1, 2)
    for k in (1, 2, 3):
        y_last(k)
        halo(k, 3)
    stat_sum(1, 3)
    end_or_both(arrived, "gh", wide_u.at[0:2])

    sums = summed_terms(1, wide_u, lambda step: stat_sum(1, step + 4))

    cross, square = total_of(1, 0) / cells, total_of(1, 1) / cells
    gap = (cross - shift * EPSILON) / (norm + EPSILON)
    residual_sq = square - 2.0 * gap * cross + gap * gap * norm
    inverse = 1.0 / jnp.sqrt(jnp.maximum(residual_sq, 0.0) + EPSILON)
    for j in range(2):
        u, sigma = next_out[j], sigma_out[j]
        next_out[j] = inverse * (u - gap * v_rows[j])
        applied = jnp.where(masks[j], energies[j] * u + scale * sums[j], 0.0)
        sigma_out[j] = inverse * (applied - gap * sigma)

    end_or_both(sent, "halo", wide_v.at[2:4])
    for run in range(2):
        sent(("relay", run), opp_tx.at[run])
        sent(("y", run), y_tx.at[run])
        sent(("z", run), z_tx.at[run])
        sent(("stat", run), stat_tx.at[run, 0 : last_stage[run]])
    sent("gz", z_tx.at[0])
    sent("gy", left.at[0, 0:2, 0:3])
    end_or_both(sent, "gh", wide_u.at[2:4])


def write_out(next_in, sigma_in, next_out, sigma_out, sem):
    pairs = ((next_in, next_out), (sigma_in, sigma_out))
    copies = [pltpu.make_async_copy(a, b, sem.at[i]) for i, (a, b) in enumerate(pairs)]
    for copy in copies:
        copy.start()
    for copy in copies:
        copy.wait()


def on_device(
    dims, lanczos_vector, left_block, right_block, left_energy, right_energy, sector_shifts, sector_sizes
):
    n_z, n_y = dims[3:]
    sectors, block, width = lanczos_vector.shape
    terms = left_block.shape[1]
    span = block // (n_z * n_y)
    strips = (n_z, n_y, span)
    out = pltpu.VMEM((sectors, span, width), F32)
    exchange = [pltpu.VMEM((2, parts, n_z, span, width), BF16) for parts in (2, 2, 4, 4)]
    vmem = pl.BlockSpec(memory_space=pltpu.VMEM)
    hbm = pl.BlockSpec(memory_space=pl.ANY)
    results = pl.pallas_call(
        functools.partial(kernel, dims),
        out_shape=(out, out),
        in_specs=[hbm] * 7,
        out_specs=(vmem, vmem),
        scratch_shapes=[
            pltpu.SMEM((terms,), jnp.int32),
            pltpu.SMEM((sectors,), jnp.int32),
            pltpu.VMEM((sectors, block), F32),
            pltpu.VMEM((sectors, width), F32),
            pltpu.VMEM((sectors, n_z * n_y, span, width), F32),
            pltpu.VMEM((sectors, span, width), F32),
            pltpu.VMEM((sectors, terms, *strips, width), BF16),
            pltpu.VMEM((sectors, terms, block, width), BF16),
            pltpu.VMEM((5, *strips, width), BF16),
            pltpu.VMEM((5, *strips, width), BF16),
            *exchange,
            pltpu.VMEM((2, n_z, span, width), F32),
            pltpu.VMEM((2, n_z, span, width), F32),
            pltpu.VMEM((2, 3, 2, span, width), BF16),
            pltpu.VMEM((2, 3, 2, span, width), BF16),
            pltpu.VMEM((2, span, width), F32),
            pltpu.VMEM((sectors, n_z * span, terms * width), BF16),
            pltpu.VMEM((sectors, terms * width, block), BF16),
            pltpu.VMEM((2, 9, 2, 8, 128), F32),
            pltpu.VMEM((2, 8, 2, 8, 128), F32),
            pltpu.SemaphoreType.DMA((9,)),
            pltpu.SemaphoreType.DMA((SOURCES,)),
            pltpu.SemaphoreType.DMA((GROUPS,)),
        ],
        compiler_params=pltpu.CompilerParams(collective_id=0, has_side_effects=True),
        name="davidson_step",
    )(
        sector_shifts,
        sector_sizes,
        left_energy,
        right_energy,
        lanczos_vector.reshape(sectors, n_z * n_y, span, width),
        left_block.reshape(sectors, terms, *strips, width),
        right_block,
    )
    whole = jax.ShapeDtypeStruct((sectors, span, width), F32)
    return pl.pallas_call(
        write_out,
        out_shape=(whole, whole),
        in_specs=[hbm, hbm],
        out_specs=(hbm, hbm),
        scratch_shapes=[pltpu.SemaphoreType.DMA((2,))],
        compiler_params=pltpu.CompilerParams(vmem_limit_bytes=1 << 20),
        name="write_out",
    )(*results)


def solution(mesh):
    dims = (2, 4, 2, 4, 4)
    finer = Mesh(mesh.devices.reshape(*dims), (*SECTOR, *TERM))
    return jax.shard_map(
        functools.partial(on_device, dims),
        mesh=finer,
        in_specs=(
            P(SECTOR, None, None),
            P(SECTOR, TERM, None, None),
            P(SECTOR, TERM, None, None),
            P(SECTOR, None),
            P(SECTOR, None),
            P(TERM),
            P(SECTOR),
        ),
        out_specs=(P(SECTOR, TERM, None), P(SECTOR, TERM, None)),
        check_vma=False,
    )
```
